8 devices in a mesh: data: 1 (over z), img: 2 (over y), seq: 4 (over x, core).
Axes of the slice: x: 2, y: 2, z: 1, core: 2. Of those that a mesh axis runs over, the one named last changes fastest.
Arguments:
- x_in: bfloat16 [2, 16384, 384], P(('data', 'img'), 'seq')
- grad_y: bfloat16 [2, 16384, 384], P(('data', 'img'), 'seq')
- ln_gamma: float32 [384], replicated
- ln_beta: float32 [384], replicated
- w_qkv: bfloat16 [384, 1152], replicated
- w_out: bfloat16 [384, 384], replicated
- head_temp: float32 [8], replicated
Outputs:
- output 1: bfloat16 [2, 16384, 384], P(('data', 'img'), 'seq')
- output 2: bfloat16 [2, 16384, 384], P(('data', 'img'), 'seq')
- output 3: float32 [384, 1152], P(('data', 'seq'))
- output 4: float32 [384, 384], P(('data', 'seq'))
- output 5: float32 [384], P('data')
- output 6: float32 [384], P('data')
- output 7: float32 [8], P('data')
All inputs are finite; a program needn't handle non-finite values.
Results may differ from the reference program's by a relative error of at most 0.00418227.
Values are sent between devices in bfloat16 or wider.
A program may use at most 1 GiB of HBM per device.

```python
import jax
import jax.numpy as jnp
from jax import lax

IMAGES = 2
TOKENS = 16384
MODEL_DIM = 384
NUM_HEADS = 8
HEAD_DIM = 48
LN_EPS = 1e-6


def layer_norm(x_f32, ln_gamma, ln_beta):
    row_mean = jnp.mean(x_f32, axis=-1, keepdims=True)
    centered = x_f32 - row_mean
    row_var = jnp.mean(centered * centered, axis=-1, keepdims=True)
    return centered * lax.rsqrt(row_var + LN_EPS) * ln_gamma + ln_beta


def attn_probs(gram_mat, sum_qq, sum_kk, head_temp):
    scale_mat = head_temp[..., :, None, None] * lax.rsqrt(sum_qq)[..., :, None] * lax.rsqrt(sum_kk)[..., None, :]
    return jax.nn.softmax(gram_mat * scale_mat, axis=-1)


def setup_inputs(seed: int = 0, part: int = 0) -> dict:
    base_key = jax.random.key(seed)
    part_key = jax.random.fold_in(base_key, part)
    k_noise, k_region, k_grad = jax.random.split(part_key, 3)
    k_gamma, k_beta, k_wqkv, k_wout, k_temp = jax.random.split(jax.random.key(seed + 1), 5)
    region_id = (jnp.arange(TOKENS) * 8) // TOKENS
    region_vec = 1.5 * jax.random.normal(k_region, (IMAGES, 8, MODEL_DIM), jnp.float32)
    noise_val = jax.random.normal(k_noise, (IMAGES, TOKENS, MODEL_DIM), jnp.float32)
    x_in = (noise_val + region_vec[:, region_id, :]).astype(jnp.bfloat16)
    grad_y = jax.random.normal(k_grad, (IMAGES, TOKENS, MODEL_DIM), jnp.float32).astype(jnp.bfloat16)
    ln_gamma = 1.0 + 0.3 * jax.random.normal(k_gamma, (MODEL_DIM,), jnp.float32)
    ln_beta = 0.5 * jax.random.normal(k_beta, (MODEL_DIM,), jnp.float32)
    fan_scale = MODEL_DIM ** -0.5
    w_qkv = (fan_scale * jax.random.normal(k_wqkv, (MODEL_DIM, 3 * MODEL_DIM), jnp.float32)).astype(jnp.bfloat16)
    w_out = (fan_scale * jax.random.normal(k_wout, (MODEL_DIM, MODEL_DIM), jnp.float32)).astype(jnp.bfloat16)
    head_temp = jax.random.uniform(k_temp, (NUM_HEADS,), jnp.float32, 4.0, 8.0)
    return {'x_in': x_in, 'grad_y': grad_y, 'ln_gamma': ln_gamma, 'ln_beta': ln_beta, 'w_qkv': w_qkv, 'w_out': w_out, 'head_temp': head_temp}


def reference(x_in, grad_y, ln_gamma, ln_beta, w_qkv, w_out, head_temp):
    def image_step(acc_sums, img_pair):
        x_img, gy_img = img_pair
        x_f32 = x_img.astype(jnp.float32)
        u_f32, ln_pull = jax.vjp(layer_norm, x_f32, ln_gamma, ln_beta)
        u_act = u_f32.astype(jnp.bfloat16)
        qkv_all = jnp.dot(u_act, w_qkv, preferred_element_type=jnp.float32).astype(jnp.bfloat16)
        qkv_heads = qkv_all.reshape(TOKENS, 3, NUM_HEADS, HEAD_DIM).astype(jnp.float32)
        q_act = qkv_heads[:, 0]
        k_act = qkv_heads[:, 1]
        v_act = qkv_heads[:, 2]
        gram_mat = jnp.einsum('nhi,nhj->hij', q_act, k_act)
        sum_qq = jnp.sum(q_act * q_act, axis=0)
        sum_kk = jnp.sum(k_act * k_act, axis=0)
        attn_p, attn_pull = jax.vjp(attn_probs, gram_mat, sum_qq, sum_kk, head_temp)
        attn_pb = attn_p.astype(jnp.bfloat16).astype(jnp.float32)
        head_out = jnp.einsum('nhj,hij->nhi', v_act, attn_pb).astype(jnp.bfloat16).reshape(TOKENS, MODEL_DIM)
        proj_out = jnp.dot(head_out, w_out, preferred_element_type=jnp.float32)
        y_img = (x_f32 + proj_out).astype(jnp.bfloat16)
        grad_wout = jnp.dot(head_out.T, gy_img, preferred_element_type=jnp.float32)
        grad_o = jnp.dot(gy_img, w_out.T, preferred_element_type=jnp.float32).astype(jnp.bfloat16)
        grad_oh = grad_o.reshape(TOKENS, NUM_HEADS, HEAD_DIM).astype(jnp.float32)
        grad_attn = jnp.einsum('nhi,nhj->hij', grad_oh, v_act)
        grad_v = jnp.einsum('nhi,hij->nhj', grad_oh, attn_pb)
        grad_gram, grad_sqq, grad_skk, grad_temp = attn_pull(grad_attn)
        gram_gb = grad_gram.astype(jnp.bfloat16).astype(jnp.float32)
        grad_q = jnp.einsum('nhj,hij->nhi', k_act, gram_gb) + 2.0 * grad_sqq * q_act
        grad_k = jnp.einsum('nhi,hij->nhj', q_act, gram_gb) + 2.0 * grad_skk * k_act
        grad_qkv = jnp.stack([grad_q, grad_k, grad_v], axis=1).reshape(TOKENS, 3 * MODEL_DIM).astype(jnp.bfloat16)
        grad_wqkv = jnp.dot(u_act.T, grad_qkv, preferred_element_type=jnp.float32)
        grad_u = jnp.dot(grad_qkv, w_qkv.T, preferred_element_type=jnp.float32).astype(jnp.bfloat16)
        grad_xln, grad_gamma, grad_beta = ln_pull(grad_u.astype(jnp.float32))
        grad_x = (gy_img.astype(jnp.float32) + grad_xln).astype(jnp.bfloat16)
        new_sums = (acc_sums[0] + grad_wqkv, acc_sums[1] + grad_wout, acc_sums[2] + grad_gamma, acc_sums[3] + grad_beta, acc_sums[4] + grad_temp)
        return new_sums, (y_img, grad_x)

    zero_sums = (jnp.zeros((MODEL_DIM, 3 * MODEL_DIM), jnp.float32), jnp.zeros((MODEL_DIM, MODEL_DIM), jnp.float32), jnp.zeros((MODEL_DIM,), jnp.float32), jnp.zeros((MODEL_DIM,), jnp.float32), jnp.zeros((NUM_HEADS,), jnp.float32))
    final_sums, (y_out, grad_x) = lax.scan(image_step, zero_sums, (x_in, grad_y))
    return y_out, grad_x, final_sums[0], final_sums[1], final_sums[2], final_sums[3], final_sums[4]
```

```python
import functools

import jax
import jax.numpy as jnp
from jax import lax
from jax.experimental import pallas as pl
from jax.experimental.pallas import tpu as pltpu
from jax.sharding import PartitionSpec as P

LN_EPS = 1e-6
MESH = pl.DeviceIdType.MESH
F32 = jnp.float32
BF16 = jnp.bfloat16

D = 384
H = 8
C = 48
SPLIT = 240
OFF = 128
ROWS = 96
TB = 512


def mm(a, b):
    return jnp.dot(a, b, preferred_element_type=F32)


def mm_nt(a, b):
    return lax.dot_general(a, b, (((1,), (1,)), ((), ())), preferred_element_type=F32)


def col_mask(h):
    col = lax.broadcasted_iota(jnp.int32, (C, D), 1)
    return (col >= C * h) & (col < C * h + C)


def to_column(row, h):
    col = lax.broadcasted_iota(jnp.int32, (C, D), 1)
    line = lax.broadcasted_iota(jnp.int32, (C, D), 0)
    return jnp.sum(jnp.where(col == line + C * h, row, 0.0), axis=1, keepdims=True)


def to_row(column, h):
    col = lax.broadcasted_iota(jnp.int32, (C, D), 1)
    line = lax.broadcasted_iota(jnp.int32, (C, D), 0)
    return jnp.sum(jnp.where(col == line + C * h, column, 0.0), axis=0, keepdims=True)


def pack(lo, hi):
    p_lo = jnp.zeros((C, 256), F32)
    p_hi = jnp.zeros((C, 256), F32)
    for h in range(5):
        p_lo += jnp.where(col_mask(h)[:, 0:256], lo[C * h : C * h + C, :], 0.0)
    for h in range(5, H):
        r = C * h - SPLIT
        p_hi += jnp.where(col_mask(h)[:, OFF:D], hi[r : r + C, :], 0.0)
    return jnp.concatenate([p_lo[:, 0:128], p_lo[:, 128:256] + p_hi[:, 0:128], p_hi[:, 128:256]], axis=1)


def block_mm(w, act):
    lo = mm(w[0:SPLIT, 0:256], act[0:256, :])
    hi = mm(w[SPLIT:D, OFF:D], act[OFF:D, :])
    return lo, hi


def kernel(
    nb,
    x_hbm, dy_hbm, gamma_ref, beta_ref, wqkv_ref, wo_ref, tau_ref,
    y_hbm, dx_hbm, gwqkv_ref, gwo_ref, ggam_ref, gbet_ref, gtau_ref,
    x_v, dy_v, y_v, ut, qkvt, dot_v, ot, mean_v, rstd_v, wqkvt,
    g_lo, g_hi, sq_acc, sk_acc, ex_g, ex_a, a_f, a_b, a_bt, dg_b, dg_bt, dsq_v, dsk_v,
    pw, ra, sa, rb, sb, rc, gb_acc, ex_gb, ex_t,
    x_sem, dy_sem, y_sem, dx_sem,
    exg_s, exg_r, exa_s, exa_r, a_s, a_r, b_s, b_r, c_s, c_r, gb_s, gb_r, t_s, t_r,
):
    data = lax.axis_index("data")
    img = lax.axis_index("img")
    seq = lax.axis_index("seq")
    xc = seq // 2
    core = seq % 2

    def dev(k):
        i = 1 - img if k & 4 else img
        xx = 1 - xc if k & 2 else xc
        cc = 1 - core if k & 1 else core
        return (data, i, xx * 2 + cc)

    barrier = pltpu.get_barrier_semaphore()
    for k in range(1, 8):
        pl.semaphore_signal(barrier, inc=1, device_id=dev(k), device_id_type=MESH)

    def x_in(t):
        return pltpu.make_async_copy(x_hbm.at[t], x_v.at[t], x_sem.at[t])

    def dy_in(t):
        return pltpu.make_async_copy(dy_hbm.at[t], dy_v.at[t], dy_sem.at[t])

    def y_out(t):
        return pltpu.make_async_copy(y_v.at[t], y_hbm.at[t], y_sem.at[t])

    def dx_out(t):
        return pltpu.make_async_copy(dy_v.at[t], dx_hbm.at[t], dx_sem.at[t])

    for t in range(nb):
        x_in(t).start()
    for t in range(nb):
        dy_in(t).start()

    def remote(src, dst, s, r, k):
        return pltpu.make_async_remote_copy(
            src_ref=src, dst_ref=dst, send_sem=s, recv_sem=r, device_id=dev(k), device_id_type=MESH
        )

    def small(buf, s, r, k):
        return remote(buf.at[0], buf.at[k], s.at[k], r.at[k], k)

    def stage_a(c, xx):
        rows = pl.ds(pl.multiple_of(ROWS * (2 * xx + 1 - core), 8), ROWS)
        return remote(pw.at[c, rows, :], ra.at[c, xx], a_s.at[c, xx], a_r.at[c, xx], 1)

    def stage_b(c):
        return remote(sa.at[c, 1 - xc], rb.at[c], b_s.at[c], b_r.at[c], 2)

    def stage_c(c):
        return remote(sb.at[c], rc.at[c], c_s.at[c], c_r.at[c], 4)

    def start_a(c):
        for xx in range(2):
            stage_a(c, xx).start()

    def start_b(c):
        for xx in range(2):
            stage_a(c, xx).wait_recv()
            rows = pl.ds(pl.multiple_of(ROWS * (2 * xx + core), 8), ROWS)
            sa[c, xx] = pw[c, rows, :] + ra[c, xx]
        stage_b(c).start()

    def start_c(c):
        stage_b(c).wait_recv()
        sb[c] = sa[c, xc] + rb[c]
        stage_c(c).start()

    wqkvt[...] = wqkv_ref[...].T
    for ref in (g_lo, g_hi, sq_acc, sk_acc, gb_acc, pw):
        ref[...] = jnp.zeros_like(ref)
    gamma = gamma_ref[...]
    beta = beta_ref[...]

    def lane_fold(a):
        out = a[:, 0:128]
        for i in range(1, TB // 128):
            out = out + a[:, 128 * i : 128 * i + 128]
        return out

    def phase1(t, carry):
        x_in(t).wait()
        x = x_v[t].astype(F32)
        mean = jnp.mean(x, axis=-1, keepdims=True)
        cen = x - mean
        var = jnp.mean(cen * cen, axis=-1, keepdims=True)
        rstd = lax.rsqrt(var + LN_EPS)
        mean_v[t] = jnp.broadcast_to(mean, (TB, 128))
        rstd_v[t] = jnp.broadcast_to(rstd, (TB, 128))
        u = (cen * rstd * gamma + beta).astype(BF16)
        u_t = u.T
        ut[t] = u_t
        qk = mm(wqkvt[0 : 2 * D, :], u_t).astype(BF16)
        qkvt[t, 0 : 2 * D, :] = qk
        q = qk[0:D, :]
        k = qk[D : 2 * D, :]
        g_lo[...] += mm_nt(q[0:SPLIT, :], k[0:256, :])
        g_hi[...] += mm_nt(q[SPLIT:D, :], k[OFF:D, :])
        qf = q.astype(F32)
        kf = k.astype(F32)
        sq_acc[...] += lane_fold(qf * qf)
        sk_acc[...] += lane_fold(kf * kf)
        return carry

    lax.fori_loop(0, nb, phase1, 0)

    ex_g[0, 0:C, :] = pack(g_lo[...], g_hi[...])
    sq_row = jnp.zeros((1, D), F32)
    sk_row = jnp.zeros((1, D), F32)
    for h in range(H):
        rows = slice(C * h, C * h + C)
        sq_row += to_row(jnp.sum(sq_acc[rows, :], axis=1, keepdims=True), h)
        sk_row += to_row(jnp.sum(sk_acc[rows, :], axis=1, keepdims=True), h)
    ex_g[0, C : C + 8, :] = jnp.concatenate([sq_row, sk_row, jnp.zeros((6, D), F32)], axis=0)
    pl.semaphore_wait(barrier, 7)
    for k in range(1, 4):
        small(ex_g, exg_s, exg_r, k).start()

    g_lo[...] = jnp.zeros_like(g_lo)
    g_hi[...] = jnp.zeros_like(g_hi)

    def phase2(t, carry):
        dy_in(t).wait()
        v = mm(wqkvt[2 * D : 3 * D, :], ut[t]).astype(BF16)
        qkvt[t, 2 * D : 3 * D, :] = v
        do = mm_nt(wo_ref[...], dy_v[t]).astype(BF16)
        dot_v[t] = do
        g_lo[...] += mm_nt(do[0:SPLIT, :], v[0:256, :])
        g_hi[...] += mm_nt(do[SPLIT:D, :], v[OFF:D, :])
        return carry

    lax.fori_loop(0, nb, phase2, 0)
    ex_a[0] = pack(g_lo[...], g_hi[...])
    for k in range(1, 4):
        small(ex_a, exa_s, exa_r, k).start()

    for k in range(1, 4):
        small(ex_g, exg_s, exg_r, k).wait_recv()
    gram_all = (ex_g[0] + ex_g[1]) + (ex_g[2] + ex_g[3])
    gram = gram_all[0:C, :]
    sq_row = gram_all[C : C + 1, :]
    sk_row = gram_all[C + 1 : C + 2, :]
    rk = lax.rsqrt(sk_row)
    for h in range(H):
        m = col_mask(h)
        rq = lax.rsqrt(to_column(sq_row, h))
        z = jnp.where(m, gram * (tau_ref[h] * rq * rk), -jnp.inf)
        e = jnp.exp(z - jnp.max(z, axis=1, keepdims=True))
        a = e / jnp.sum(e, axis=1, keepdims=True)
        a_f[h] = a
        a_b[C * h : C * h + C, :] = a.astype(BF16)
    a_bt[...] = a_b[...].T

    def phase3(t, carry):
        o_lo, o_hi = block_mm(a_b[...], qkvt[t, 2 * D : 3 * D, :])
        ot[t, 0:SPLIT, :] = o_lo.astype(BF16)
        ot[t, SPLIT:D, :] = o_hi.astype(BF16)
        pw[0] += mm(ot[t], dy_v[t])
        return carry

    lax.fori_loop(0, nb, phase3, 0)
    start_a(0)

    def phase4(t, carry):
        dv_lo, dv_hi = block_mm(a_bt[...], dot_v[t])
        qkvt[t, 2 * D : 2 * D + SPLIT, :] = dv_lo.astype(BF16)
        qkvt[t, 2 * D + SPLIT : 3 * D, :] = dv_hi.astype(BF16)
        pw[1] += mm_nt(ut[t], qkvt[t, 2 * D : 3 * D, :])

        @pl.when(t == 3)
        def _():
            start_b(0)

        return carry

    lax.fori_loop(0, nb, phase4, 0)
    start_a(1)

    for k in range(1, 4):
        small(ex_a, exa_s, exa_r, k).wait_recv()
    d_attn = (ex_a[0] + ex_a[1]) + (ex_a[2] + ex_a[3])
    drk = jnp.zeros((1, D), F32)
    lane = lax.broadcasted_iota(jnp.int32, (8, 128), 1)
    dtau = jnp.zeros((8, 128), F32)
    for h in range(H):
        m = col_mask(h)
        tau = tau_ref[h]
        sq = to_column(sq_row, h)
        rq = lax.rsqrt(sq)
        a = a_f[h]
        da = jnp.where(m, d_attn, 0.0)
        dz = a * (da - jnp.sum(da * a, axis=1, keepdims=True))
        dg_b[C * h : C * h + C, :] = jnp.where(m, dz * (tau * rq * rk), 0.0).astype(BF16)
        w = dz * gram
        wrk = jnp.sum(jnp.where(m, w * rk, 0.0), axis=1, keepdims=True)
        dsq = (tau * wrk) * (-0.5 * (rq / sq))
        dsq_v[C * h : C * h + C, :] = jnp.broadcast_to(2.0 * dsq, (C, 128))
        drk += jnp.sum(jnp.where(m, w * (tau * rq), 0.0), axis=0, keepdims=True)
        dtau += jnp.where(lane == h, jnp.sum(wrk * rq), 0.0)
    dsk = drk * (-0.5 * (rk / sk_row))
    for h in range(H):
        dsk_v[C * h : C * h + C, :] = jnp.broadcast_to(2.0 * to_column(dsk, h), (C, 128))
    dg_bt[...] = dg_b[...].T
    ex_t[0] = dtau
    t_copy = remote(ex_t.at[0], ex_t.at[1], t_s, t_r, 4)
    t_copy.start()

    def phase5(t, carry):
        q = qkvt[t, 0:D, :]
        k = qkvt[t, D : 2 * D, :]
        dq_lo, dq_hi = block_mm(dg_b[...], k)
        dk_lo, dk_hi = block_mm(dg_bt[...], q)
        qf = q.astype(F32)
        kf = k.astype(F32)
        ds = dsq_v[:, 0:1]
        dk = dsk_v[:, 0:1]
        qkvt[t, 0:SPLIT, :] = (dq_lo + ds[0:SPLIT] * qf[0:SPLIT]).astype(BF16)
        qkvt[t, SPLIT:D, :] = (dq_hi + ds[SPLIT:D] * qf[SPLIT:D]).astype(BF16)
        qkvt[t, D : D + SPLIT, :] = (dk_lo + dk[0:SPLIT] * kf[0:SPLIT]).astype(BF16)
        qkvt[t, D + SPLIT : 2 * D, :] = (dk_hi + dk[SPLIT:D] * kf[SPLIT:D]).astype(BF16)
        dw = mm_nt(ut[t], qkvt[t, 0 : 2 * D, :])
        pw[2] += dw[:, 0:D]
        pw[3] += dw[:, D : 2 * D]

        @pl.when(t == 1)
        def _():
            start_b(1)

        @pl.when(t == 6)
        def _():
            start_c(0)

        return carry

    lax.fori_loop(0, nb, phase5, 0)
    start_a(2)
    start_a(3)

    def phase6(t, carry):
        x = x_v[t].astype(F32)
        dy = dy_v[t].astype(F32)
        y_v[t] = (x + mm(ot[t].T, wo_ref[...])).astype(BF16)
        y_out(t).start()
        du_t = mm(wqkv_ref[...], qkvt[t]).astype(BF16)
        du = du_t.T.astype(F32)
        rstd = rstd_v[t][:, 0:1]
        xhat = (x - mean_v[t][:, 0:1]) * rstd
        g = du * gamma
        m1 = jnp.mean(g, axis=-1, keepdims=True)
        m2 = jnp.mean(g * xhat, axis=-1, keepdims=True)
        dx = rstd * (g - m1 - xhat * m2)
        dy_v[t] = (dy + dx).astype(BF16)
        dx_out(t).start()
        dgam = jnp.sum((du * xhat).reshape(TB // 8, 8, D), axis=0)
        dbet = jnp.sum(du.reshape(TB // 8, 8, D), axis=0)
        gb_acc[0] += dgam
        gb_acc[1] += dbet

        @pl.when(t == 1)
        def _():
            start_b(2)
            start_c(1)

        @pl.when(t == 3)
        def _():
            start_b(3)

        @pl.when(t == 5)
        def _():
            start_c(2)

        @pl.when(t == 7)
        def _():
            start_c(3)

        return carry

    lax.fori_loop(0, nb, phase6, 0)

    dgam = jnp.sum(gb_acc[0], axis=0, keepdims=True)
    dbet = jnp.sum(gb_acc[1], axis=0, keepdims=True)
    ex_gb[0] = jnp.concatenate([dgam, dbet, jnp.zeros((6, D), F32)], axis=0)
    for k in range(1, 8):
        small(ex_gb, gb_s, gb_r, k).start()

    for c in range(4):
        stage_c(c).wait_recv()
        total = sb[c] + rc[c]
        if c == 0:
            gwo_ref[...] = total
        else:
            col = {1: 2 * D, 2: 0, 3: D}[c]
            gwqkv_ref[:, col : col + D] = total
    t_copy.wait_recv()
    gtau_ref[...] = (ex_t[0] + ex_t[1])[0:1, 0:H]
    for k in range(1, 8):
        small(ex_gb, gb_s, gb_r, k).wait_recv()
    gb = ((ex_gb[0] + ex_gb[1]) + (ex_gb[2] + ex_gb[3])) + ((ex_gb[4] + ex_gb[5]) + (ex_gb[6] + ex_gb[7]))
    ggam_ref[...] = gb[0:1, :]
    gbet_ref[...] = gb[1:2, :]

    for t in range(nb):
        y_out(t).wait()
        dx_out(t).wait()
    for k in range(1, 4):
        small(ex_g, exg_s, exg_r, k).wait_send()
        small(ex_a, exa_s, exa_r, k).wait_send()
    for c in range(4):
        for xx in range(2):
            stage_a(c, xx).wait_send()
        stage_b(c).wait_send()
        stage_c(c).wait_send()
    t_copy.wait_send()
    for k in range(1, 8):
        small(ex_gb, gb_s, gb_r, k).wait_send()


def solution(mesh):
    act_spec = P(("data", "img"), "seq", None)
    row_spec = P(("data", "seq"), None)
    in_specs = (act_spec, act_spec, P(), P(), P(), P(), P())
    out_specs = (act_spec, act_spec, row_spec, row_spec, P("data"), P("data"), P("data"))

    def local_block(x_in, grad_y, ln_gamma, ln_beta, w_qkv, w_out, head_temp):
        n_tok = x_in.shape[1]
        nb = n_tok // TB
        hbm = pl.BlockSpec(memory_space=pl.ANY)
        vmem = pl.BlockSpec(memory_space=pltpu.VMEM)
        smem = pl.BlockSpec(memory_space=pltpu.SMEM)
        dma = pltpu.SemaphoreType.DMA
        outs = pl.pallas_call(
            functools.partial(kernel, nb),
            out_shape=(
                jax.ShapeDtypeStruct((nb, TB, D), BF16),
                jax.ShapeDtypeStruct((nb, TB, D), BF16),
                jax.ShapeDtypeStruct((ROWS, 3 * D), F32),
                jax.ShapeDtypeStruct((ROWS, D), F32),
                jax.ShapeDtypeStruct((1, D), F32),
                jax.ShapeDtypeStruct((1, D), F32),
                jax.ShapeDtypeStruct((1, H), F32),
            ),
            in_specs=[hbm, hbm, vmem, vmem, vmem, vmem, smem],
            out_specs=(hbm, hbm, vmem, vmem, vmem, vmem, vmem),
            scratch_shapes=[
                pltpu.VMEM((nb, TB, D), BF16),
                pltpu.VMEM((nb, TB, D), BF16),
                pltpu.VMEM((nb, TB, D), BF16),
                pltpu.VMEM((nb, D, TB), BF16),
                pltpu.VMEM((nb, 3 * D, TB), BF16),
                pltpu.VMEM((nb, D, TB), BF16),
                pltpu.VMEM((nb, D, TB), BF16),
                pltpu.VMEM((nb, TB, 128), F32),
                pltpu.VMEM((nb, TB, 128), F32),
                pltpu.VMEM((3 * D, D), BF16),
                pltpu.VMEM((SPLIT, 256), F32),
                pltpu.VMEM((D - SPLIT, 256), F32),
                pltpu.VMEM((D, 128), F32),
                pltpu.VMEM((D, 128), F32),
                pltpu.VMEM((4, C + 8, D), F32),
                pltpu.VMEM((4, C, D), F32),
                pltpu.VMEM((H, C, D), F32),
                pltpu.VMEM((D, D), BF16),
                pltpu.VMEM((D, D), BF16),
                pltpu.VMEM((D, D), BF16),
                pltpu.VMEM((D, D), BF16),
                pltpu.VMEM((D, 128), F32),
                pltpu.VMEM((D, 128), F32),
                pltpu.VMEM((4, D, D), F32),
                pltpu.VMEM((4, 2, ROWS, D), F32),
                pltpu.VMEM((4, 2, ROWS, D), F32),
                pltpu.VMEM((4, ROWS, D), F32),
                pltpu.VMEM((4, ROWS, D), F32),
                pltpu.VMEM((4, ROWS, D), F32),
                pltpu.VMEM((2, 8, D), F32),
                pltpu.VMEM((8, 8, D), F32),
                pltpu.VMEM((2, 8, 128), F32),
                dma((nb,)), dma((nb,)), dma((nb,)), dma((nb,)),
                dma((4,)), dma((4,)), dma((4,)), dma((4,)),
                dma((4, 2)), dma((4, 2)), dma((4,)), dma((4,)), dma((4,)), dma((4,)),
                dma((8,)), dma((8,)), dma, dma,
            ],
            compiler_params=pltpu.CompilerParams(
                collective_id=0, has_side_effects=True, vmem_limit_bytes=64000000
            ),
            name="xca_block",
        )(
            x_in.reshape(nb, TB, D),
            grad_y.reshape(nb, TB, D),
            ln_gamma.reshape(1, D),
            ln_beta.reshape(1, D),
            w_qkv,
            w_out,
            head_temp,
        )
        y, dx, gwqkv, gwo, ggam, gbet, gtau = outs
        return (
            y.reshape(1, n_tok, D),
            dx.reshape(1, n_tok, D),
            gwqkv,
            gwo,
            ggam.reshape(D),
            gbet.reshape(D),
            gtau.reshape(H),
        )

    return jax.shard_map(local_block, mesh=mesh, in_specs=in_specs, out_specs=out_specs, check_vma=False)
```

```python
import functools

import jax
import jax.numpy as jnp
from jax import lax
from jax.experimental import pallas as pl
from jax.experimental.pallas import tpu as pltpu
from jax.sharding import PartitionSpec as P

LN_EPS = 1e-6
MESH = pl.DeviceIdType.MESH
F32 = jnp.float32
BF16 = jnp.bfloat16

D = 384
H = 8
C = 48
SPLIT = 240
OFF = 128
ROWS = 96
TB = 1024
S4B0 = 1
S5B1 = 0
S5C0 = 3
S6B2 = 0
S6B3 = 1
S6C2 = 2
S6C3 = 3


def mm(a, b):
    return jnp.dot(a, b, preferred_element_type=F32)


def mm_nt(a, b):
    return lax.dot_general(a, b, (((1,), (1,)), ((), ())), preferred_element_type=F32)


def col_mask(h):
    col = lax.broadcasted_iota(jnp.int32, (C, D), 1)
    return (col >= C * h) & (col < C * h + C)


def to_column(row, h):
    col = lax.broadcasted_iota(jnp.int32, (C, D), 1)
    line = lax.broadcasted_iota(jnp.int32, (C, D), 0)
    return jnp.sum(jnp.where(col == line + C * h, row, 0.0), axis=1, keepdims=True)


def to_row(column, h):
    col = lax.broadcasted_iota(jnp.int32, (C, D), 1)
    line = lax.broadcasted_iota(jnp.int32, (C, D), 0)
    return jnp.sum(jnp.where(col == line + C * h, column, 0.0), axis=0, keepdims=True)


def pack(lo, hi):
    p_lo = jnp.zeros((C, 256), F32)
    p_hi = jnp.zeros((C, 256), F32)
    for h in range(5):
        p_lo += jnp.where(col_mask(h)[:, 0:256], lo[C * h : C * h + C, :], 0.0)
    for h in range(5, H):
        r = C * h - SPLIT
        p_hi += jnp.where(col_mask(h)[:, OFF:D], hi[r : r + C, :], 0.0)
    return jnp.concatenate([p_lo[:, 0:128], p_lo[:, 128:256] + p_hi[:, 0:128], p_hi[:, 128:256]], axis=1)


def block_mm(w, act):
    lo = mm(w[0:SPLIT, 0:256], act[0:256, :])
    hi = mm(w[SPLIT:D, OFF:D], act[OFF:D, :])
    return lo, hi


def kernel(
    nb,
    x_hbm, dy_hbm, gamma_ref, beta_ref, wqkv_ref, wo_ref, tau_ref,
    y_v, dx_v, gwqkv_ref, gwo_ref, ggam_ref, gbet_ref, gtau_ref,
    x_v, dy_v, ut, qkvt, dot_v, ot, mean_v, rstd_v, wqkvt,
    g_lo, g_hi, sq_acc, sk_acc, ex_g, ex_a, a_f, a_b, a_bt, dg_b, dg_bt, dsq_v, dsk_v,
    pw, ra, sa, rb, sb, rc, gb_acc, ex_gb, ex_t,
    x_sem, dy_sem,
    exg_s, exg_r, exa_s, exa_r, a_s, a_r, b_s, b_r, c_s, c_r, gb_s, gb_r, t_s, t_r,
):
    data = lax.axis_index("data")
    img = lax.axis_index("img")
    seq = lax.axis_index("seq")
    xc = seq // 2
    core = seq % 2

    def dev(k):
        i = 1 - img if k & 4 else img
        xx = 1 - xc if k & 2 else xc
        cc = 1 - core if k & 1 else core
        return (data, i, xx * 2 + cc)

    barrier = pltpu.get_barrier_semaphore()
    for k in range(1, 8):
        pl.semaphore_signal(barrier, inc=1, device_id=dev(k), device_id_type=MESH)

    def x_in(t):
        return pltpu.make_async_copy(x_hbm.at[t], x_v.at[t], x_sem.at[t])

    def dy_in(t):
        return pltpu.make_async_copy(dy_hbm.at[t], dy_v.at[t], dy_sem.at[t])

    for t in range(nb):
        x_in(t).start()
    for t in range(nb):
        dy_in(t).start()

    def remote(src, dst, s, r, k):
        return pltpu.make_async_remote_copy(
            src_ref=src, dst_ref=dst, send_sem=s, recv_sem=r, device_id=dev(k), device_id_type=MESH
        )

    def small(buf, s, r, k):
        return remote(buf.at[0], buf.at[k], s.at[k], r.at[k], k)

    def stage_a(c, xx):
        rows = pl.ds(pl.multiple_of(ROWS * (2 * xx + 1 - core), 8), ROWS)
        return remote(pw.at[c, rows, :], ra.at[c, xx], a_s.at[c, xx], a_r.at[c, xx], 1)

    def stage_b(c):
        return remote(sa.at[c, 1 - xc], rb.at[c], b_s.at[c], b_r.at[c], 2)

    def stage_c(c):
        return remote(sb.at[c], rc.at[c], c_s.at[c], c_r.at[c], 4)

    def start_a(c):
        for xx in range(2):
            stage_a(c, xx).start()

    def start_b(c):
        for xx in range(2):
            stage_a(c, xx).wait_recv()
            rows = pl.ds(pl.multiple_of(ROWS * (2 * xx + core), 8), ROWS)
            sa[c, xx] = pw[c, rows, :] + ra[c, xx]
        stage_b(c).start()

    def start_c(c):
        stage_b(c).wait_recv()
        sb[c] = sa[c, xc] + rb[c]
        stage_c(c).start()

    wqkvt[...] = wqkv_ref[...].T
    for ref in (g_lo, g_hi, sq_acc, sk_acc, gb_acc, pw):
        ref[...] = jnp.zeros_like(ref)
    gamma = gamma_ref[...].reshape(1, D)
    beta = beta_ref[...].reshape(1, D)

    def lane_fold(a):
        out = a[:, 0:128]
        for i in range(1, TB // 128):
            out = out + a[:, 128 * i : 128 * i + 128]
        return out

    def phase1(t, carry):
        x_in(t).wait()
        x = x_v[t].astype(F32)
        mean = jnp.mean(x, axis=-1, keepdims=True)
        cen = x - mean
        var = jnp.mean(cen * cen, axis=-1, keepdims=True)
        rstd = lax.rsqrt(var + LN_EPS)
        mean_v[t] = jnp.broadcast_to(mean, (TB, 128))
        rstd_v[t] = jnp.broadcast_to(rstd, (TB, 128))
        u = (cen * rstd * gamma + beta).astype(BF16)
        u_t = u.T
        ut[t] = u_t
        qk = mm(wqkvt[0 : 2 * D, :], u_t).astype(BF16)
        qkvt[t, 0 : 2 * D, :] = qk
        q = qk[0:D, :]
        k = qk[D : 2 * D, :]
        g_lo[...] += mm_nt(q[0:SPLIT, :], k[0:256, :])
        g_hi[...] += mm_nt(q[SPLIT:D, :], k[OFF:D, :])
        qf = q.astype(F32)
        kf = k.astype(F32)
        sq_acc[...] += lane_fold(qf * qf)
        sk_acc[...] += lane_fold(kf * kf)
        return carry

    lax.fori_loop(0, nb, phase1, 0)

    ex_g[0, 0:C, :] = pack(g_lo[...], g_hi[...])
    sq_row = jnp.zeros((1, D), F32)
    sk_row = jnp.zeros((1, D), F32)
    for h in range(H):
        rows = slice(C * h, C * h + C)
        sq_row += to_row(jnp.sum(sq_acc[rows, :], axis=1, keepdims=True), h)
        sk_row += to_row(jnp.sum(sk_acc[rows, :], axis=1, keepdims=True), h)
    ex_g[0, C : C + 8, :] = jnp.concatenate([sq_row, sk_row, jnp.zeros((6, D), F32)], axis=0)
    pl.semaphore_wait(barrier, 7)
    for k in range(1, 4):
        small(ex_g, exg_s, exg_r, k).start()

    g_lo[...] = jnp.zeros_like(g_lo)
    g_hi[...] = jnp.zeros_like(g_hi)

    def phase2(t, carry):
        dy_in(t).wait()
        v = mm(wqkvt[2 * D : 3 * D, :], ut[t]).astype(BF16)
        qkvt[t, 2 * D : 3 * D, :] = v
        do = mm_nt(wo_ref[...], dy_v[t]).astype(BF16)
        dot_v[t] = do
        g_lo[...] += mm_nt(do[0:SPLIT, :], v[0:256, :])
        g_hi[...] += mm_nt(do[SPLIT:D, :], v[OFF:D, :])
        return carry

    lax.fori_loop(0, nb, phase2, 0)
    ex_a[0] = pack(g_lo[...], g_hi[...])
    for k in range(1, 4):
        small(ex_a, exa_s, exa_r, k).start()

    for k in range(1, 4):
        small(ex_g, exg_s, exg_r, k).wait_recv()
    gram_all = (ex_g[0] + ex_g[1]) + (ex_g[2] + ex_g[3])
    gram = gram_all[0:C, :]
    sq_row = gram_all[C : C + 1, :]
    sk_row = gram_all[C + 1 : C + 2, :]
    rk = lax.rsqrt(sk_row)
    for h in range(H):
        m = col_mask(h)
        rq = lax.rsqrt(to_column(sq_row, h))
        z = jnp.where(m, gram * (tau_ref[h] * rq * rk), -jnp.inf)
        e = jnp.exp(z - jnp.max(z, axis=1, keepdims=True))
        a = e / jnp.sum(e, axis=1, keepdims=True)
        a_f[h] = a
        a_b[C * h : C * h + C, :] = a.astype(BF16)
    a_bt[...] = a_b[...].T

    def phase3(t, carry):
        o_lo, o_hi = block_mm(a_b[...], qkvt[t, 2 * D : 3 * D, :])
        ot[t, 0:SPLIT, :] = o_lo.astype(BF16)
        ot[t, SPLIT:D, :] = o_hi.astype(BF16)
        pw[0] += mm(ot[t], dy_v[t])
        return carry

    lax.fori_loop(0, nb, phase3, 0)
    start_a(0)

    def phase4(t, carry):
        dv_lo, dv_hi = block_mm(a_bt[...], dot_v[t])
        qkvt[t, 2 * D : 2 * D + SPLIT, :] = dv_lo.astype(BF16)
        qkvt[t, 2 * D + SPLIT : 3 * D, :] = dv_hi.astype(BF16)
        pw[1] += mm_nt(ut[t], qkvt[t, 2 * D : 3 * D, :])

        @pl.when(t == S4B0)
        def _():
            start_b(0)

        return carry

    lax.fori_loop(0, nb, phase4, 0)
    start_a(1)

    for k in range(1, 4):
        small(ex_a, exa_s, exa_r, k).wait_recv()
    d_attn = (ex_a[0] + ex_a[1]) + (ex_a[2] + ex_a[3])
    drk = jnp.zeros((1, D), F32)
    lane = lax.broadcasted_iota(jnp.int32, (8, 128), 1)
    dtau = jnp.zeros((8, 128), F32)
    for h in range(H):
        m = col_mask(h)
        tau = tau_ref[h]
        sq = to_column(sq_row, h)
        rq = lax.rsqrt(sq)
        a = a_f[h]
        da = jnp.where(m, d_attn, 0.0)
        dz = a * (da - jnp.sum(da * a, axis=1, keepdims=True))
        dg_b[C * h : C * h + C, :] = jnp.where(m, dz * (tau * rq * rk), 0.0).astype(BF16)
        w = dz * gram
        wrk = jnp.sum(jnp.where(m, w * rk, 0.0), axis=1, keepdims=True)
        dsq = (tau * wrk) * (-0.5 * (rq / sq))
        dsq_v[C * h : C * h + C, :] = jnp.broadcast_to(2.0 * dsq, (C, 128))
        drk += jnp.sum(jnp.where(m, w * (tau * rq), 0.0), axis=0, keepdims=True)
        dtau += jnp.where(lane == h, jnp.sum(wrk * rq), 0.0)
    dsk = drk * (-0.5 * (rk / sk_row))
    for h in range(H):
        dsk_v[C * h : C * h + C, :] = jnp.broadcast_to(2.0 * to_column(dsk, h), (C, 128))
    dg_bt[...] = dg_b[...].T
    ex_t[0] = dtau
    t_copy = remote(ex_t.at[0], ex_t.at[1], t_s, t_r, 4)
    t_copy.start()

    def phase5(t, carry):
        q = qkvt[t, 0:D, :]
        k = qkvt[t, D : 2 * D, :]
        dq_lo, dq_hi = block_mm(dg_b[...], k)
        dk_lo, dk_hi = block_mm(dg_bt[...], q)
        qf = q.astype(F32)
        kf = k.astype(F32)
        ds = dsq_v[:, 0:1]
        dk = dsk_v[:, 0:1]
        qkvt[t, 0:SPLIT, :] = (dq_lo + ds[0:SPLIT] * qf[0:SPLIT]).astype(BF16)
        qkvt[t, SPLIT:D, :] = (dq_hi + ds[SPLIT:D] * qf[SPLIT:D]).astype(BF16)
        qkvt[t, D : D + SPLIT, :] = (dk_lo + dk[0:SPLIT] * kf[0:SPLIT]).astype(BF16)
        qkvt[t, D + SPLIT : 2 * D, :] = (dk_hi + dk[SPLIT:D] * kf[SPLIT:D]).astype(BF16)
        dw = mm_nt(ut[t], qkvt[t, 0 : 2 * D, :])
        pw[2] += dw[:, 0:D]
        pw[3] += dw[:, D : 2 * D]

        @pl.when(t == S5B1)
        def _():
            start_b(1)

        @pl.when(t == S5C0)
        def _():
            start_c(0)

        return carry

    lax.fori_loop(0, nb, phase5, 0)
    start_a(2)
    start_a(3)

    def phase6(t, carry):
        x = x_v[t].astype(F32)
        dy = dy_v[t].astype(F32)
        y_v[t] = (x + mm(ot[t].T, wo_ref[...])).astype(BF16)
        du_t = mm(wqkv_ref[...], qkvt[t]).astype(BF16)
        du = du_t.T.astype(F32)
        rstd = rstd_v[t][:, 0:1]
        xhat = (x - mean_v[t][:, 0:1]) * rstd
        g = du * gamma
        m1 = jnp.mean(g, axis=-1, keepdims=True)
        m2 = jnp.mean(g * xhat, axis=-1, keepdims=True)
        dx = rstd * (g - m1 - xhat * m2)
        dx_v[t] = (dy + dx).astype(BF16)
        dgam = jnp.sum((du * xhat).reshape(TB // 8, 8, D), axis=0)
        dbet = jnp.sum(du.reshape(TB // 8, 8, D), axis=0)
        gb_acc[0] += dgam
        gb_acc[1] += dbet

        @pl.when(t == S6B2)
        def _():
            start_b(2)
            start_c(1)

        @pl.when(t == S6B3)
        def _():
            start_b(3)

        @pl.when(t == S6C2)
        def _():
            start_c(2)

        @pl.when(t == S6C3)
        def _():
            start_c(3)

        return carry

    lax.fori_loop(0, nb, phase6, 0)

    dgam = jnp.sum(gb_acc[0], axis=0, keepdims=True)
    dbet = jnp.sum(gb_acc[1], axis=0, keepdims=True)
    ex_gb[0] = jnp.concatenate([dgam, dbet, jnp.zeros((6, D), F32)], axis=0)
    for k in range(1, 8):
        small(ex_gb, gb_s, gb_r, k).start()

    for c in range(4):
        stage_c(c).wait_recv()
        total = sb[c] + rc[c]
        if c == 0:
            gwo_ref[...] = total
        else:
            col = {1: 2 * D, 2: 0, 3: D}[c]
            gwqkv_ref[:, col : col + D] = total
    t_copy.wait_recv()
    gtau_ref[...] = (ex_t[0] + ex_t[1])[0, 0:H]
    for k in range(1, 8):
        small(ex_gb, gb_s, gb_r, k).wait_recv()
    gb = ((ex_gb[0] + ex_gb[1]) + (ex_gb[2] + ex_gb[3])) + ((ex_gb[4] + ex_gb[5]) + (ex_gb[6] + ex_gb[7]))
    ggam_ref[...] = gb[0]
    gbet_ref[...] = gb[1]

    for k in range(1, 4):
        small(ex_g, exg_s, exg_r, k).wait_send()
        small(ex_a, exa_s, exa_r, k).wait_send()
    for c in range(4):
        for xx in range(2):
            stage_a(c, xx).wait_send()
        stage_b(c).wait_send()
        stage_c(c).wait_send()
    t_copy.wait_send()
    for k in range(1, 8):
        small(ex_gb, gb_s, gb_r, k).wait_send()


def store_kernel(*refs):
    sem = refs[14]
    copies = [pltpu.make_async_copy(refs[i], refs[7 + i], sem.at[i]) for i in range(7)]
    for copy in copies:
        copy.start()
    for copy in copies:
        copy.wait()


def solution(mesh):
    act_spec = P(("data", "img"), "seq", None)
    row_spec = P(("data", "seq"), None)
    in_specs = (act_spec, act_spec, P(), P(), P(), P(), P())
    out_specs = (act_spec, act_spec, row_spec, row_spec, P("data"), P("data"), P("data"))

    def local_block(x_in, grad_y, ln_gamma, ln_beta, w_qkv, w_out, head_temp):
        n_tok = x_in.shape[1]
        nb = n_tok // TB
        hbm = pl.BlockSpec(memory_space=pl.ANY)
        vmem = pl.BlockSpec(memory_space=pltpu.VMEM)
        smem = pl.BlockSpec(memory_space=pltpu.SMEM)
        dma = pltpu.SemaphoreType.DMA
        outs = pl.pallas_call(
            functools.partial(kernel, nb),
            out_shape=(
                pltpu.VMEM((nb, TB, D), BF16),
                pltpu.VMEM((nb, TB, D), BF16),
                pltpu.VMEM((ROWS, 3 * D), F32),
                pltpu.VMEM((ROWS, D), F32),
                pltpu.VMEM((D,), F32),
                pltpu.VMEM((D,), F32),
                pltpu.VMEM((H,), F32),
            ),
            in_specs=[hbm, hbm, vmem, vmem, vmem, vmem, smem],
            out_specs=(vmem,) * 7,
            scratch_shapes=[
                pltpu.VMEM((nb, TB, D), BF16),
                pltpu.VMEM((nb, TB, D), BF16),
                pltpu.VMEM((nb, D, TB), BF16),
                pltpu.VMEM((nb, 3 * D, TB), BF16),
                pltpu.VMEM((nb, D, TB), BF16),
                pltpu.VMEM((nb, D, TB), BF16),
                pltpu.VMEM((nb, TB, 128), F32),
                pltpu.VMEM((nb, TB, 128), F32),
                pltpu.VMEM((3 * D, D), BF16),
                pltpu.VMEM((SPLIT, 256), F32),
                pltpu.VMEM((D - SPLIT, 256), F32),
                pltpu.VMEM((D, 128), F32),
                pltpu.VMEM((D, 128), F32),
                pltpu.VMEM((4, C + 8, D), F32),
                pltpu.VMEM((4, C, D), F32),
                pltpu.VMEM((H, C, D), F32),
                pltpu.VMEM((D, D), BF16),
                pltpu.VMEM((D, D), BF16),
                pltpu.VMEM((D, D), BF16),
                pltpu.VMEM((D, D), BF16),
                pltpu.VMEM((D, 128), F32),
                pltpu.VMEM((D, 128), F32),
                pltpu.VMEM((4, D, D), F32),
                pltpu.VMEM((4, 2, ROWS, D), F32),
                pltpu.VMEM((4, 2, ROWS, D), F32),
                pltpu.VMEM((4, ROWS, D), F32),
                pltpu.VMEM((4, ROWS, D), F32),
                pltpu.VMEM((4, ROWS, D), F32),
                pltpu.VMEM((2, 8, D), F32),
                pltpu.VMEM((8, 8, D), F32),
                pltpu.VMEM((2, 8, 128), F32),
                dma((nb,)), dma((nb,)),
                dma((4,)), dma((4,)), dma((4,)), dma((4,)),
                dma((4, 2)), dma((4, 2)), dma((4,)), dma((4,)), dma((4,)), dma((4,)),
                dma((8,)), dma((8,)), dma, dma,
            ],
            compiler_params=pltpu.CompilerParams(
                collective_id=0, has_side_effects=True, vmem_limit_bytes=52000000
            ),
            name="xca_block",
        )(
            x_in.reshape(nb, TB, D),
            grad_y.reshape(nb, TB, D),
            ln_gamma,
            ln_beta,
            w_qkv,
            w_out,
            head_temp,
        )
        outs = pl.pallas_call(
            store_kernel,
            out_shape=(
                jax.ShapeDtypeStruct((nb, TB, D), BF16),
                jax.ShapeDtypeStruct((nb, TB, D), BF16),
                jax.ShapeDtypeStruct((ROWS, 3 * D), F32),
                jax.ShapeDtypeStruct((ROWS, D), F32),
                jax.ShapeDtypeStruct((D,), F32),
                jax.ShapeDtypeStruct((D,), F32),
                jax.ShapeDtypeStruct((H,), F32),
            ),
            in_specs=[hbm] * 7,
            out_specs=(hbm,) * 7,
            scratch_shapes=[dma((7,))],
            compiler_params=pltpu.CompilerParams(vmem_limit_bytes=4 * 2**20),
            name="xca_store",
        )(*outs)
        y, dx, gwqkv, gwo, ggam, gbet, gtau = outs
        return y.reshape(1, n_tok, D), dx.reshape(1, n_tok, D), gwqkv, gwo, ggam, gbet, gtau

    return jax.shard_map(local_block, mesh=mesh, in_specs=in_specs, out_specs=out_specs, check_vma=False)
```

```python
import functools

import jax
import jax.numpy as jnp
from jax import lax
from jax.experimental import pallas as pl
from jax.experimental.pallas import tpu as pltpu
from jax.sharding import PartitionSpec as P

LN_EPS = 1e-6
MESH = pl.DeviceIdType.MESH
F32 = jnp.float32
BF16 = jnp.bfloat16

D = 384
H = 8
C = 48
SPLIT = 240
OFF = 128
ROWS = 96
TB = 1024
HALVES = (1, 1, 1, 2)


def mm(a, b):
    return jnp.dot(a, b, preferred_element_type=F32)


def mm_nt(a, b):
    return lax.dot_general(a, b, (((1,), (1,)), ((), ())), preferred_element_type=F32)


def col_mask(h):
    col = lax.broadcasted_iota(jnp.int32, (C, D), 1)
    return (col >= C * h) & (col < C * h + C)


def to_column(row, h):
    col = lax.broadcasted_iota(jnp.int32, (C, D), 1)
    line = lax.broadcasted_iota(jnp.int32, (C, D), 0)
    return jnp.sum(jnp.where(col == line + C * h, row, 0.0), axis=1, keepdims=True)


def to_row(column, h):
    col = lax.broadcasted_iota(jnp.int32, (C, D), 1)
    line = lax.broadcasted_iota(jnp.int32, (C, D), 0)
    return jnp.sum(jnp.where(col == line + C * h, column, 0.0), axis=0, keepdims=True)


def pack(lo, hi):
    p_lo = jnp.zeros((C, 256), F32)
    p_hi = jnp.zeros((C, 256), F32)
    for h in range(5):
        p_lo += jnp.where(col_mask(h)[:, 0:256], lo[C * h : C * h + C, :], 0.0)
    for h in range(5, H):
        r = C * h - SPLIT
        p_hi += jnp.where(col_mask(h)[:, OFF:D], hi[r : r + C, :], 0.0)
    return jnp.concatenate([p_lo[:, 0:128], p_lo[:, 128:256] + p_hi[:, 0:128], p_hi[:, 128:256]], axis=1)


def block_mm(w, act):
    lo = mm(w[0:SPLIT, 0:256], act[0:256, :])
    hi = mm(w[SPLIT:D, OFF:D], act[OFF:D, :])
    return lo, hi


def kernel(
    nb,
    x_hbm, dy_hbm, gamma_hbm, beta_hbm, wqkv_hbm, wo_hbm, tau_hbm,
    y_v, dx_v, gwqkv_ref, gwo_ref, ggam_ref, gbet_ref, gtau_ref,
    x_v, dy_v, ut, qkvt, dot_v, ot, mean_v, rstd_v, wqkvt,
    gamma_ref, beta_ref, wqkv_ref, wo_ref, tau_ref,
    g_lo, g_hi, sq_acc, sk_acc, ex_g, ex_h, ex_a, a_f, a_b, a_bt, dg_b, dg_bt, dsq_v, dsk_v,
    pw, ra, sa, rb, sb, rc, gb_acc, ex_gb, ex_t,
    x_sem, dy_sem, in_sem,
    exg_s, exg_r, exa_s, exa_r, a_s, a_r, b_s, b_r, c_s, c_r, gb_s, gb_r, t_s, t_r,
):
    data = lax.axis_index("data")
    img = lax.axis_index("img")
    seq = lax.axis_index("seq")
    xc = seq // 2
    core = seq % 2

    def dev(k):
        i = 1 - img if k & 4 else img
        xx = 1 - xc if k & 2 else xc
        cc = 1 - core if k & 1 else core
        return (data, i, xx * 2 + cc)

    barrier = pltpu.get_barrier_semaphore()
    for k in range(1, 8):
        pl.semaphore_signal(barrier, inc=1, device_id=dev(k), device_id_type=MESH)

    def x_in(t):
        return pltpu.make_async_copy(x_hbm.at[t], x_v.at[t], x_sem.at[t])

    def dy_in(t):
        return pltpu.make_async_copy(dy_hbm.at[t], dy_v.at[t], dy_sem.at[t])

    def weight_in(i):
        pairs = ((wqkv_hbm, wqkv_ref), (gamma_hbm, gamma_ref), (beta_hbm, beta_ref), (wo_hbm, wo_ref), (tau_hbm, tau_ref))
        return pltpu.make_async_copy(*pairs[i], in_sem.at[i])

    weight_in(0).start()
    for t in range(nb):
        x_in(t).start()
    for i in range(1, 5):
        weight_in(i).start()
    for t in range(nb):
        dy_in(t).start()

    def remote(src, dst, s, r, k):
        return pltpu.make_async_remote_copy(
            src_ref=src, dst_ref=dst, send_sem=s, recv_sem=r, device_id=dev(k), device_id_type=MESH
        )

    def small(buf, s, r, k):
        return remote(buf.at[0], buf.at[k], s.at[k], r.at[k], k)

    def stage_a(c, xx):
        rows = pl.ds(pl.multiple_of(ROWS * (2 * xx + 1 - core), 8), ROWS)
        return remote(pw.at[c, rows, :], ra.at[c, xx], a_s.at[c, xx], a_r.at[c, xx], 1)

    def part(c, h):
        return pl.ds(h * (ROWS // HALVES[c]), ROWS // HALVES[c])

    def stage_b(c, h):
        return remote(sa.at[c, 1 - xc, part(c, h)], rb.at[c, part(c, h)], b_s.at[c, h], b_r.at[c, h], 2)

    def stage_c(c, h):
        return remote(sb.at[c, part(c, h)], rc.at[c, part(c, h)], c_s.at[c, h], c_r.at[c, h], 4)

    def start_a(c):
        for xx in range(2):
            stage_a(c, xx).start()

    def start_b(c):
        for xx in range(2):
            stage_a(c, xx).wait_recv()
            rows = pl.ds(pl.multiple_of(ROWS * (2 * xx + core), 8), ROWS)
            sa[c, xx] = pw[c, rows, :] + ra[c, xx]
        for h in range(HALVES[c]):
            stage_b(c, h).start()

    def start_c(c, h=0):
        stage_b(c, h).wait_recv()
        sb[c, part(c, h)] = sa[c, xc, part(c, h)] + rb[c, part(c, h)]
        stage_c(c, h).start()

    def loop(body, steps):
        for t in range(nb):
            body(t)
            if (t + 1) * 4 % nb == 0 and (t + 1) * 4 // nb - 1 in steps:
                steps[(t + 1) * 4 // nb - 1]()

    for ref in (g_lo, g_hi, sq_acc, sk_acc, gb_acc, pw):
        ref[...] = jnp.zeros_like(ref)
    for i in range(3):
        weight_in(i).wait()
    wqkvt[...] = wqkv_ref[...].T
    gamma = gamma_ref[...].reshape(1, D)
    beta = beta_ref[...].reshape(1, D)

    def lane_fold(a):
        out = a[:, 0:128]
        for i in range(1, TB // 128):
            out = out + a[:, 128 * i : 128 * i + 128]
        return out

    def phase1(t):
        x_in(t).wait()
        x = x_v[t].astype(F32)
        mean = jnp.mean(x, axis=-1, keepdims=True)
        cen = x - mean
        var = jnp.mean(cen * cen, axis=-1, keepdims=True)
        rstd = lax.rsqrt(var + LN_EPS)
        mean_v[t] = jnp.broadcast_to(mean, (TB, 128))
        rstd_v[t] = jnp.broadcast_to(rstd, (TB, 128))
        u = (cen * rstd * gamma + beta).astype(BF16)
        u_t = u.T
        ut[t] = u_t
        qk = mm(wqkvt[0 : 2 * D, :], u_t).astype(BF16)
        qkvt[t, 0 : 2 * D, :] = qk
        q = qk[0:D, :]
        k = qk[D : 2 * D, :]
        g_lo[...] += mm_nt(q[0:SPLIT, :], k[0:256, :])
        g_hi[...] += mm_nt(q[SPLIT:D, :], k[OFF:D, :])
        qf = q.astype(F32)
        kf = k.astype(F32)
        sq_acc[...] += lane_fold(qf * qf)
        sk_acc[...] += lane_fold(kf * kf)

    loop(phase1, {})

    ex_g[0, 0:C, :] = pack(g_lo[...], g_hi[...])
    sq_row = jnp.zeros((1, D), F32)
    sk_row = jnp.zeros((1, D), F32)
    for h in range(H):
        rows = slice(C * h, C * h + C)
        sq_row += to_row(jnp.sum(sq_acc[rows, :], axis=1, keepdims=True), h)
        sk_row += to_row(jnp.sum(sk_acc[rows, :], axis=1, keepdims=True), h)
    ex_g[0, C : C + 8, :] = jnp.concatenate([sq_row, sk_row, jnp.zeros((6, D), F32)], axis=0)
    pl.semaphore_wait(barrier, 7)
    g_core = remote(ex_g.at[0], ex_g.at[1], exg_s.at[0], exg_r.at[0], 1)
    g_chip = remote(ex_h.at[0], ex_h.at[1], exg_s.at[1], exg_r.at[1], 2)
    g_core.start()
    for i in range(3, 5):
        weight_in(i).wait()

    def gram_step():
        g_core.wait_recv()
        ex_h[0] = ex_g[0] + ex_g[1]
        g_chip.start()

    g_lo[...] = jnp.zeros_like(g_lo)
    g_hi[...] = jnp.zeros_like(g_hi)

    def phase2(t):
        dy_in(t).wait()
        v = mm(wqkvt[2 * D : 3 * D, :], ut[t]).astype(BF16)
        qkvt[t, 2 * D : 3 * D, :] = v
        do = mm_nt(wo_ref[...], dy_v[t]).astype(BF16)
        dot_v[t] = do
        g_lo[...] += mm_nt(do[0:SPLIT, :], v[0:256, :])
        g_hi[...] += mm_nt(do[SPLIT:D, :], v[OFF:D, :])

    loop(phase2, {0: gram_step})
    ex_a[0] = pack(g_lo[...], g_hi[...])
    for k in range(1, 4):
        small(ex_a, exa_s, exa_r, k).start()

    g_chip.wait_recv()
    gram_all = ex_h[0] + ex_h[1]
    gram = gram_all[0:C, :]
    sq_row = gram_all[C : C + 1, :]
    sk_row = gram_all[C + 1 : C + 2, :]
    rk = lax.rsqrt(sk_row)
    for h in range(H):
        m = col_mask(h)
        rq = lax.rsqrt(to_column(sq_row, h))
        z = jnp.where(m, gram * (tau_ref[h] * rq * rk), -jnp.inf)
        e = jnp.exp(z - jnp.max(z, axis=1, keepdims=True))
        a = e / jnp.sum(e, axis=1, keepdims=True)
        a_f[h] = a
        a_b[C * h : C * h + C, :] = a.astype(BF16)
    a_bt[...] = a_b[...].T

    def phase3(t):
        o_lo, o_hi = block_mm(a_b[...], qkvt[t, 2 * D : 3 * D, :])
        ot[t, 0:SPLIT, :] = o_lo.astype(BF16)
        ot[t, SPLIT:D, :] = o_hi.astype(BF16)
        pw[0] += mm(ot[t], dy_v[t])

    loop(phase3, {})
    start_a(0)

    def phase4(t):
        dv_lo, dv_hi = block_mm(a_bt[...], dot_v[t])
        qkvt[t, 2 * D : 2 * D + SPLIT, :] = dv_lo.astype(BF16)
        qkvt[t, 2 * D + SPLIT : 3 * D, :] = dv_hi.astype(BF16)
        pw[1] += mm_nt(ut[t], qkvt[t, 2 * D : 3 * D, :])

    loop(phase4, {1: lambda: start_b(0)})
    start_a(1)

    for k in range(1, 4):
        small(ex_a, exa_s, exa_r, k).wait_recv()
    d_attn = (ex_a[0] + ex_a[1]) + (ex_a[2] + ex_a[3])
    drk = jnp.zeros((1, D), F32)
    lane = lax.broadcasted_iota(jnp.int32, (8, 128), 1)
    dtau = jnp.zeros((8, 128), F32)
    for h in range(H):
        m = col_mask(h)
        tau = tau_ref[h]
        sq = to_column(sq_row, h)
        rq = lax.rsqrt(sq)
        a = a_f[h]
        da = jnp.where(m, d_attn, 0.0)
        dz = a * (da - jnp.sum(da * a, axis=1, keepdims=True))
        dg_b[C * h : C * h + C, :] = jnp.where(m, dz * (tau * rq * rk), 0.0).astype(BF16)
        w = dz * gram
        wrk = jnp.sum(jnp.where(m, w * rk, 0.0), axis=1, keepdims=True)
        dsq = (tau * wrk) * (-0.5 * (rq / sq))
        dsq_v[C * h : C * h + C, :] = jnp.broadcast_to(2.0 * dsq, (C, 128))
        drk += jnp.sum(jnp.where(m, w * (tau * rq), 0.0), axis=0, keepdims=True)
        dtau += jnp.where(lane == h, jnp.sum(wrk * rq), 0.0)
    dsk = drk * (-0.5 * (rk / sk_row))
    for h in range(H):
        dsk_v[C * h : C * h + C, :] = jnp.broadcast_to(2.0 * to_column(dsk, h), (C, 128))
    dg_bt[...] = dg_b[...].T
    ex_t[0] = dtau
    t_copy = remote(ex_t.at[0], ex_t.at[1], t_s, t_r, 4)
    t_copy.start()

    def phase5(t):
        dq_lo, dq_hi = block_mm(dg_b[...], qkvt[t, D : 2 * D, :])
        qf = qkvt[t, 0:D, :].astype(F32)
        ds = dsq_v[:, 0:1]
        dot_v[t, 0:SPLIT, :] = (dq_lo + ds[0:SPLIT] * qf[0:SPLIT]).astype(BF16)
        dot_v[t, SPLIT:D, :] = (dq_hi + ds[SPLIT:D] * qf[SPLIT:D]).astype(BF16)
        pw[2] += mm_nt(ut[t], dot_v[t])

    loop(phase5, {0: lambda: start_b(1), 3: lambda: start_c(0)})
    start_a(2)

    def phase6(t):
        dk_lo, dk_hi = block_mm(dg_bt[...], qkvt[t, 0:D, :])
        kf = qkvt[t, D : 2 * D, :].astype(F32)
        ds = dsk_v[:, 0:1]
        qkvt[t, D : D + SPLIT, :] = (dk_lo + ds[0:SPLIT] * kf[0:SPLIT]).astype(BF16)
        qkvt[t, D + SPLIT : 2 * D, :] = (dk_hi + ds[SPLIT:D] * kf[SPLIT:D]).astype(BF16)
        pw[3] += mm_nt(ut[t], qkvt[t, D : 2 * D, :])

    loop(phase6, {1: lambda: start_b(2), 2: lambda: start_c(1)})
    start_a(3)

    def phase7(t):
        du_t = mm(wqkv_ref[:, 0:D], dot_v[t]) + mm(wqkv_ref[:, D : 3 * D], qkvt[t, D : 3 * D, :])
        du = du_t.astype(BF16).T.astype(F32)
        rstd = rstd_v[t][:, 0:1]
        xhat = (x_v[t].astype(F32) - mean_v[t][:, 0:1]) * rstd
        g = du * gamma
        m1 = jnp.mean(g, axis=-1, keepdims=True)
        m2 = jnp.mean(g * xhat, axis=-1, keepdims=True)
        dx = rstd * (g - m1 - xhat * m2)
        dx_v[t] = (dy_v[t].astype(F32) + dx).astype(BF16)
        gb_acc[0] += jnp.sum((du * xhat).reshape(TB // 8, 8, D), axis=0)
        gb_acc[1] += jnp.sum(du.reshape(TB // 8, 8, D), axis=0)

    loop(
        phase7,
        {
            0: lambda: start_b(3),
            1: lambda: start_c(2),
            2: lambda: start_c(3, 0),
            3: lambda: start_c(3, 1),
        })

    dgam = jnp.sum(gb_acc[0], axis=0, keepdims=True)
    dbet = jnp.sum(gb_acc[1], axis=0, keepdims=True)
    ex_gb[0] = jnp.concatenate([dgam, dbet, jnp.zeros((6, D), F32)], axis=0)
    for k in range(1, 8):
        small(ex_gb, gb_s, gb_r, k).start()

    def phase8(t):
        y_v[t] = (x_v[t].astype(F32) + mm(ot[t].T, wo_ref[...])).astype(BF16)

    loop(phase8, {})

    for c in range(4):
        for h in range(HALVES[c]):
            stage_c(c, h).wait_recv()
        total = sb[c] + rc[c]
        if c == 0:
            gwo_ref[...] = total
        else:
            col = {1: 2 * D, 2: 0, 3: D}[c]
            gwqkv_ref[:, col : col + D] = total
    t_copy.wait_recv()
    gtau_ref[...] = (ex_t[0] + ex_t[1])[0, 0:H]
    for k in range(1, 8):
        small(ex_gb, gb_s, gb_r, k).wait_recv()
    gb = ((ex_gb[0] + ex_gb[1]) + (ex_gb[2] + ex_gb[3])) + ((ex_gb[4] + ex_gb[5]) + (ex_gb[6] + ex_gb[7]))
    ggam_ref[...] = gb[0]
    gbet_ref[...] = gb[1]

    for k in range(1, 4):
        small(ex_a, exa_s, exa_r, k).wait_send()
    for c in range(4):
        for xx in range(2):
            stage_a(c, xx).wait_send()
        for h in range(HALVES[c]):
            stage_b(c, h).wait_send()
            stage_c(c, h).wait_send()
    g_core.wait_send()
    g_chip.wait_send()
    t_copy.wait_send()
    for k in range(1, 8):
        small(ex_gb, gb_s, gb_r, k).wait_send()


def store_kernel(*refs):
    sem = refs[14]
    copies = [pltpu.make_async_copy(refs[i], refs[7 + i], sem.at[i]) for i in range(7)]
    for copy in copies:
        copy.start()
    for copy in copies:
        copy.wait()


def solution(mesh):
    act_spec = P(("data", "img"), "seq", None)
    row_spec = P(("data", "seq"), None)
    in_specs = (act_spec, act_spec, P(), P(), P(), P(), P())
    out_specs = (act_spec, act_spec, row_spec, row_spec, P("data"), P("data"), P("data"))

    def local_block(x_in, grad_y, ln_gamma, ln_beta, w_qkv, w_out, head_temp):
        n_tok = x_in.shape[1]
        nb = n_tok // TB
        hbm = pl.BlockSpec(memory_space=pl.ANY)
        vmem = pl.BlockSpec(memory_space=pltpu.VMEM)
        dma = pltpu.SemaphoreType.DMA
        outs = pl.pallas_call(
            functools.partial(kernel, nb),
            out_shape=(
                pltpu.VMEM((nb, TB, D), BF16),
                pltpu.VMEM((nb, TB, D), BF16),
                pltpu.VMEM((ROWS, 3 * D), F32),
                pltpu.VMEM((ROWS, D), F32),
                pltpu.VMEM((D,), F32),
                pltpu.VMEM((D,), F32),
                pltpu.VMEM((H,), F32),
            ),
            in_specs=[hbm] * 7,
            out_specs=(vmem,) * 7,
            scratch_shapes=[
                pltpu.VMEM((nb, TB, D), BF16),
                pltpu.VMEM((nb, TB, D), BF16),
                pltpu.VMEM((nb, D, TB), BF16),
                pltpu.VMEM((nb, 3 * D, TB), BF16),
                pltpu.VMEM((nb, D, TB), BF16),
                pltpu.VMEM((nb, D, TB), BF16),
                pltpu.VMEM((nb, TB, 128), F32),
                pltpu.VMEM((nb, TB, 128), F32),
                pltpu.VMEM((3 * D, D), BF16),
                pltpu.VMEM((D,), F32),
                pltpu.VMEM((D,), F32),
                pltpu.VMEM((D, 3 * D), BF16),
                pltpu.VMEM((D, D), BF16),
                pltpu.SMEM((H,), F32),
                pltpu.VMEM((SPLIT, 256), F32),
                pltpu.VMEM((D - SPLIT, 256), F32),
                pltpu.VMEM((D, 128), F32),
                pltpu.VMEM((D, 128), F32),
                pltpu.VMEM((2, C + 8, D), F32),
                pltpu.VMEM((2, C + 8, D), F32),
                pltpu.VMEM((4, C, D), F32),
                pltpu.VMEM((H, C, D), F32),
                pltpu.VMEM((D, D), BF16),
                pltpu.VMEM((D, D), BF16),
                pltpu.VMEM((D, D), BF16),
                pltpu.VMEM((D, D), BF16),
                pltpu.VMEM((D, 128), F32),
                pltpu.VMEM((D, 128), F32),
                pltpu.VMEM((4, D, D), F32),
                pltpu.VMEM((4, 2, ROWS, D), F32),
                pltpu.VMEM((4, 2, ROWS, D), F32),
                pltpu.VMEM((4, ROWS, D), F32),
                pltpu.VMEM((4, ROWS, D), F32),
                pltpu.VMEM((4, ROWS, D), F32),
                pltpu.VMEM((2, 8, D), F32),
                pltpu.VMEM((8, 8, D), F32),
                pltpu.VMEM((2, 8, 128), F32),
                dma((nb,)), dma((nb,)), dma((5,)),
                dma((2,)), dma((2,)), dma((4,)), dma((4,)),
                dma((4, 2)), dma((4, 2)), dma((4, 2)), dma((4, 2)), dma((4, 2)), dma((4, 2)),
                dma((8,)), dma((8,)), dma, dma,
            ],
            compiler_params=pltpu.CompilerParams(
                collective_id=0, has_side_effects=True, vmem_limit_bytes=52000000
            ),
            name="xca_block",
        )(
            x_in.reshape(nb, TB, D),
            grad_y.reshape(nb, TB, D),
            ln_gamma,
            ln_beta,
            w_qkv,
            w_out,
            head_temp,
        )
        outs = pl.pallas_call(
            store_kernel,
            out_shape=(
                jax.ShapeDtypeStruct((nb, TB, D), BF16),
                jax.ShapeDtypeStruct((nb, TB, D), BF16),
                jax.ShapeDtypeStruct((ROWS, 3 * D), F32),
                jax.ShapeDtypeStruct((ROWS, D), F32),
                jax.ShapeDtypeStruct((D,), F32),
                jax.ShapeDtypeStruct((D,), F32),
                jax.ShapeDtypeStruct((H,), F32),
            ),
            in_specs=[hbm] * 7,
            out_specs=(hbm,) * 7,
            scratch_shapes=[dma((7,))],
            compiler_params=pltpu.CompilerParams(vmem_limit_bytes=4 * 2**20),
            name="xca_store",
        )(*outs)
        y, dx, gwqkv, gwo, ggam, gbet, gtau = outs
        return y.reshape(1, n_tok, D), dx.reshape(1, n_tok, D), gwqkv, gwo, ggam, gbet, gtau

    return jax.shard_map(local_block, mesh=mesh, in_specs=in_specs, out_specs=out_specs, check_vma=False)
```

```python
import functools

import jax
import jax.numpy as jnp
from jax import lax
from jax.experimental import pallas as pl
from jax.experimental.pallas import tpu as pltpu
from jax.sharding import PartitionSpec as P

LN_EPS = 1e-6
MESH = pl.DeviceIdType.MESH
F32 = jnp.float32
BF16 = jnp.bfloat16

D = 384
H = 8
C = 48
SPLIT = 240
OFF = 128
ROWS = 96
TB = 1024
PIECES = (1, 1, 1, 1)
STEPS = {
    (4, 3): [("b", 0, 0)],
    (5, 2): [("b", 1, 0)],
    (6, 2): [("c", 0, 0), ("b", 2, 0)],
    (7, 1, 0): [("b", 3, 0), ("c", 1, 0)],
    (7, 2, 0): [("c", 2, 0)],
    (7, 3, 1): [("c", 3, 0)],
}


def mm(a, b):
    return jnp.dot(a, b, preferred_element_type=F32)


def mm_nt(a, b):
    return lax.dot_general(a, b, (((1,), (1,)), ((), ())), preferred_element_type=F32)


def col_mask(h):
    col = lax.broadcasted_iota(jnp.int32, (C, D), 1)
    return (col >= C * h) & (col < C * h + C)


def to_column(row, h):
    col = lax.broadcasted_iota(jnp.int32, (C, D), 1)
    line = lax.broadcasted_iota(jnp.int32, (C, D), 0)
    return jnp.sum(jnp.where(col == line + C * h, row, 0.0), axis=1, keepdims=True)


def to_row(column, h):
    col = lax.broadcasted_iota(jnp.int32, (C, D), 1)
    line = lax.broadcasted_iota(jnp.int32, (C, D), 0)
    return jnp.sum(jnp.where(col == line + C * h, column, 0.0), axis=0, keepdims=True)


def pack(lo, hi):
    p_lo = jnp.zeros((C, 256), F32)
    p_hi = jnp.zeros((C, 256), F32)
    for h in range(5):
        p_lo += jnp.where(col_mask(h)[:, 0:256], lo[C * h : C * h + C, :], 0.0)
    for h in range(5, H):
        r = C * h - SPLIT
        p_hi += jnp.where(col_mask(h)[:, OFF:D], hi[r : r + C, :], 0.0)
    return jnp.concatenate([p_lo[:, 0:128], p_lo[:, 128:256] + p_hi[:, 0:128], p_hi[:, 128:256]], axis=1)


def block_mm(w, act):
    lo = mm(w[0:SPLIT, 0:256], act[0:256, :])
    hi = mm(w[SPLIT:D, OFF:D], act[OFF:D, :])
    return lo, hi


def kernel(
    nb,
    x_hbm, dy_hbm, gamma_hbm, beta_hbm, wqkv_hbm, wo_hbm, tau_hbm,
    y_v, dx_v, gwqkv_ref, gwo_ref, ggam_ref, gbet_ref, gtau_ref,
    x_v, dy_v, ut, qkvt, dot_v, ot, mean_v, rstd_v, wqkvt,
    gamma_ref, beta_ref, wqkv_ref, wo_ref, tau_ref,
    g_lo, g_hi, sq_acc, sk_acc, ex_g, ex_h, ex_a, a_f, a_b, a_bt, dg_b, dg_bt, dsq_v, dsk_v,
    pw, ra, sa, rb, sb, rc, gb_acc, ex_gb, ex_t,
    x_sem, dy_sem, in_sem,
    exg_s, exg_r, exa_s, exa_r, a_s, a_r, b_s, b_r, c_s, c_r, gb_s, gb_r, t_s, t_r,
):
    data = lax.axis_index("data")
    img = lax.axis_index("img")
    seq = lax.axis_index("seq")
    xc = seq // 2
    core = seq % 2

    def dev(k):
        i = 1 - img if k & 4 else img
        xx = 1 - xc if k & 2 else xc
        cc = 1 - core if k & 1 else core
        return (data, i, xx * 2 + cc)

    barrier = pltpu.get_barrier_semaphore()
    for k in range(1, 8):
        pl.semaphore_signal(barrier, inc=1, device_id=dev(k), device_id_type=MESH)

    def x_in(t):
        return pltpu.make_async_copy(x_hbm.at[t], x_v.at[t], x_sem.at[t])

    def dy_in(t):
        return pltpu.make_async_copy(dy_hbm.at[t], dy_v.at[t], dy_sem.at[t])

    def weight_in(i):
        pairs = ((wqkv_hbm, wqkv_ref), (gamma_hbm, gamma_ref), (beta_hbm, beta_ref), (wo_hbm, wo_ref), (tau_hbm, tau_ref))
        return pltpu.make_async_copy(*pairs[i], in_sem.at[i])

    weight_in(0).start()
    x_in(0).start()
    for i in range(1, 5):
        weight_in(i).start()

    def remote(src, dst, s, r, k):
        return pltpu.make_async_remote_copy(
            src_ref=src, dst_ref=dst, send_sem=s, recv_sem=r, device_id=dev(k), device_id_type=MESH
        )

    def small(buf, s, r, k):
        return remote(buf.at[0], buf.at[k], s.at[k], r.at[k], k)

    def stage_a(c, xx):
        rows = pl.ds(pl.multiple_of(ROWS * (2 * xx + 1 - core), 8), ROWS)
        return remote(pw.at[c, rows, :], ra.at[c, xx], a_s.at[c, xx], a_r.at[c, xx], 1)

    def part(c, h):
        return pl.ds(h * (ROWS // PIECES[c]), ROWS // PIECES[c])

    def stage_b(c, h):
        return remote(sa.at[c, 1 - xc, part(c, h)], rb.at[c, part(c, h)], b_s.at[c, h], b_r.at[c, h], 2)

    def stage_c(c, h):
        return remote(sb.at[c, part(c, h)], rc.at[c, part(c, h)], c_s.at[c, h], c_r.at[c, h], 4)

    def start_a(c):
        for xx in range(2):
            stage_a(c, xx).start()

    def start_b(c):
        for xx in range(2):
            stage_a(c, xx).wait_recv()
            rows = pl.ds(pl.multiple_of(ROWS * (2 * xx + core), 8), ROWS)
            sa[c, xx] = pw[c, rows, :] + ra[c, xx]
        for h in range(PIECES[c]):
            stage_b(c, h).start()

    def start_c(c, h):
        stage_b(c, h).wait_recv()
        sb[c, part(c, h)] = sa[c, xc, part(c, h)] + rb[c, part(c, h)]
        stage_c(c, h).start()

    def total(product):
        out = product(0)
        for t in range(1, nb):
            out = out + product(t)
        return out

    def go_on(*at):
        for stage, c, h in STEPS.get(at, ()):
            if stage == "b":
                start_b(c)
            else:
                start_c(c, h)

    for ref in (g_lo, g_hi, sq_acc, sk_acc, gb_acc):
        ref[...] = jnp.zeros_like(ref)
    for i in range(3):
        weight_in(i).wait()
    wqkvt[...] = wqkv_ref[...].T
    gamma = gamma_ref[...].reshape(1, D)
    beta = beta_ref[...].reshape(1, D)

    def lane_fold(a):
        out = a[:, 0:128]
        for i in range(1, TB // 128):
            out = out + a[:, 128 * i : 128 * i + 128]
        return out

    def phase1(t):
        x_in(t).wait()
        if t + 1 < nb:
            x_in(t + 1).start()
        else:
            for n in range(nb):
                dy_in(n).start()
        x = x_v[t].astype(F32)
        mean = jnp.mean(x, axis=-1, keepdims=True)
        cen = x - mean
        var = jnp.mean(cen * cen, axis=-1, keepdims=True)
        rstd = lax.rsqrt(var + LN_EPS)
        mean_v[t] = jnp.broadcast_to(mean, (TB, 128))
        rstd_v[t] = jnp.broadcast_to(rstd, (TB, 128))
        u = (cen * rstd * gamma + beta).astype(BF16)
        u_t = u.T
        ut[t] = u_t
        qk = mm(wqkvt[0 : 2 * D, :], u_t).astype(BF16)
        qkvt[t, 0 : 2 * D, :] = qk
        q = qk[0:D, :]
        k = qk[D : 2 * D, :]
        g_lo[...] += mm_nt(q[0:SPLIT, :], k[0:256, :])
        g_hi[...] += mm_nt(q[SPLIT:D, :], k[OFF:D, :])
        qf = q.astype(F32)
        kf = k.astype(F32)
        sq_acc[...] += lane_fold(qf * qf)
        sk_acc[...] += lane_fold(kf * kf)

    for t in range(nb):
        phase1(t)

    ex_g[0, 0:C, :] = pack(g_lo[...], g_hi[...])
    sq_row = jnp.zeros((1, D), F32)
    sk_row = jnp.zeros((1, D), F32)
    for h in range(H):
        rows = slice(C * h, C * h + C)
        sq_row += to_row(jnp.sum(sq_acc[rows, :], axis=1, keepdims=True), h)
        sk_row += to_row(jnp.sum(sk_acc[rows, :], axis=1, keepdims=True), h)
    ex_g[0, C : C + 8, :] = jnp.concatenate([sq_row, sk_row, jnp.zeros((6, D), F32)], axis=0)
    pl.semaphore_wait(barrier, 7)
    g_core = remote(ex_g.at[0], ex_g.at[1], exg_s.at[0], exg_r.at[0], 1)
    g_chip = remote(ex_h.at[0], ex_h.at[1], exg_s.at[1], exg_r.at[1], 2)
    g_core.start()
    for i in range(3, 5):
        weight_in(i).wait()

    def gram_step():
        g_core.wait_recv()
        ex_h[0] = ex_g[0] + ex_g[1]
        g_chip.start()

    g_lo[...] = jnp.zeros_like(g_lo)
    g_hi[...] = jnp.zeros_like(g_hi)

    def phase2(t):
        dy_in(t).wait()
        v = mm(wqkvt[2 * D : 3 * D, :], ut[t]).astype(BF16)
        qkvt[t, 2 * D : 3 * D, :] = v
        do = mm_nt(wo_ref[...], dy_v[t]).astype(BF16)
        dot_v[t] = do
        g_lo[...] += mm_nt(do[0:SPLIT, :], v[0:256, :])
        g_hi[...] += mm_nt(do[SPLIT:D, :], v[OFF:D, :])

    for t in range(nb):
        phase2(t)
        if t == 0:
            gram_step()
    ex_a[0] = pack(g_lo[...], g_hi[...])
    for k in range(1, 4):
        small(ex_a, exa_s, exa_r, k).start()

    g_chip.wait_recv()
    gram_all = ex_h[0] + ex_h[1]
    gram = gram_all[0:C, :]
    sq_row = gram_all[C : C + 1, :]
    sk_row = gram_all[C + 1 : C + 2, :]
    rk = lax.rsqrt(sk_row)
    for h in range(H):
        m = col_mask(h)
        rq = lax.rsqrt(to_column(sq_row, h))
        z = jnp.where(m, gram * (tau_ref[h] * rq * rk), -jnp.inf)
        e = jnp.exp(z - jnp.max(z, axis=1, keepdims=True))
        a = e / jnp.sum(e, axis=1, keepdims=True)
        a_f[h] = a
        a_b[C * h : C * h + C, :] = a.astype(BF16)
    a_bt[...] = a_b[...].T

    def phase3(t):
        o_lo, o_hi = block_mm(a_b[...], qkvt[t, 2 * D : 3 * D, :])
        ot[t, 0:SPLIT, :] = o_lo.astype(BF16)
        ot[t, SPLIT:D, :] = o_hi.astype(BF16)

    for t in range(nb):
        phase3(t)
    pw[0] = total(lambda t: mm(ot[t], dy_v[t]))
    start_a(0)

    def phase4(t):
        dv_lo, dv_hi = block_mm(a_bt[...], dot_v[t])
        qkvt[t, 2 * D : 2 * D + SPLIT, :] = dv_lo.astype(BF16)
        qkvt[t, 2 * D + SPLIT : 3 * D, :] = dv_hi.astype(BF16)

    for t in range(nb):
        phase4(t)
    go_on(4, 0)
    pw[1, :, 0:256] = total(lambda t: mm_nt(ut[t], qkvt[t, 2 * D : 2 * D + 256, :]))
    go_on(4, 1)
    pw[1, :, 256:D] = total(lambda t: mm_nt(ut[t], qkvt[t, 2 * D + 256 : 3 * D, :]))
    go_on(4, 2)
    start_a(1)

    for k in range(1, 4):
        small(ex_a, exa_s, exa_r, k).wait_recv()
    go_on(4, 3)
    d_attn = (ex_a[0] + ex_a[1]) + (ex_a[2] + ex_a[3])
    drk = jnp.zeros((1, D), F32)
    lane = lax.broadcasted_iota(jnp.int32, (8, 128), 1)
    dtau = jnp.zeros((8, 128), F32)
    for h in range(H):
        m = col_mask(h)
        tau = tau_ref[h]
        sq = to_column(sq_row, h)
        rq = lax.rsqrt(sq)
        a = a_f[h]
        da = jnp.where(m, d_attn, 0.0)
        dz = a * (da - jnp.sum(da * a, axis=1, keepdims=True))
        dg_b[C * h : C * h + C, :] = jnp.where(m, dz * (tau * rq * rk), 0.0).astype(BF16)
        w = dz * gram
        wrk = jnp.sum(jnp.where(m, w * rk, 0.0), axis=1, keepdims=True)
        dsq = (tau * wrk) * (-0.5 * (rq / sq))
        dsq_v[C * h : C * h + C, :] = jnp.broadcast_to(2.0 * dsq, (C, 128))
        drk += jnp.sum(jnp.where(m, w * (tau * rq), 0.0), axis=0, keepdims=True)
        dtau += jnp.where(lane == h, jnp.sum(wrk * rq), 0.0)
    dsk = drk * (-0.5 * (rk / sk_row))
    for h in range(H):
        dsk_v[C * h : C * h + C, :] = jnp.broadcast_to(2.0 * to_column(dsk, h), (C, 128))
    dg_bt[...] = dg_b[...].T
    ex_t[0] = dtau
    t_copy = remote(ex_t.at[0], ex_t.at[1], t_s, t_r, 4)
    t_copy.start()

    def phase5(t):
        dq_lo, dq_hi = block_mm(dg_b[...], qkvt[t, D : 2 * D, :])
        qf = qkvt[t, 0:D, :].astype(F32)
        ds = dsq_v[:, 0:1]
        dot_v[t, 0:SPLIT, :] = (dq_lo + ds[0:SPLIT] * qf[0:SPLIT]).astype(BF16)
        dot_v[t, SPLIT:D, :] = (dq_hi + ds[SPLIT:D] * qf[SPLIT:D]).astype(BF16)

    for t in range(nb):
        phase5(t)
    go_on(5, 0)
    pw[2, :, 0:256] = total(lambda t: mm_nt(ut[t], dot_v[t, 0:256, :]))
    go_on(5, 1)
    pw[2, :, 256:D] = total(lambda t: mm_nt(ut[t], dot_v[t, 256:D, :]))
    go_on(5, 2)
    start_a(2)

    def phase6(t):
        dk_lo, dk_hi = block_mm(dg_bt[...], qkvt[t, 0:D, :])
        kf = qkvt[t, D : 2 * D, :].astype(F32)
        ds = dsk_v[:, 0:1]
        qkvt[t, D : D + SPLIT, :] = (dk_lo + ds[0:SPLIT] * kf[0:SPLIT]).astype(BF16)
        qkvt[t, D + SPLIT : 2 * D, :] = (dk_hi + ds[SPLIT:D] * kf[SPLIT:D]).astype(BF16)

    for t in range(nb):
        phase6(t)
    go_on(6, 0)
    pw[3, :, 0:256] = total(lambda t: mm_nt(ut[t], qkvt[t, D : D + 256, :]))
    go_on(6, 1)
    pw[3, :, 256:D] = total(lambda t: mm_nt(ut[t], qkvt[t, D + 256 : 2 * D, :]))
    go_on(6, 2)
    start_a(3)

    def phase7(t, half):
        rows = slice(half * (TB // 2), (half + 1) * (TB // 2))
        du_t = mm(wqkv_ref[:, 0:D], dot_v[t, :, rows]) + mm(wqkv_ref[:, D : 3 * D], qkvt[t, D : 3 * D, rows])
        du = du_t.astype(BF16).T.astype(F32)
        rstd = rstd_v[t, rows, 0:1]
        xhat = (x_v[t, rows].astype(F32) - mean_v[t, rows, 0:1]) * rstd
        g = du * gamma
        m1 = jnp.mean(g, axis=-1, keepdims=True)
        m2 = jnp.mean(g * xhat, axis=-1, keepdims=True)
        dx = rstd * (g - m1 - xhat * m2)
        dx_v[t, rows] = (dy_v[t, rows].astype(F32) + dx).astype(BF16)
        gb_acc[0] += jnp.sum((du * xhat).reshape(TB // 16, 8, D), axis=0)
        gb_acc[1] += jnp.sum(du.reshape(TB // 16, 8, D), axis=0)

    for t in range(nb):
        for half in range(2):
            phase7(t, half)
            go_on(7, t, half)

    dgam = jnp.sum(gb_acc[0], axis=0, keepdims=True)
    dbet = jnp.sum(gb_acc[1], axis=0, keepdims=True)
    ex_gb[0] = jnp.concatenate([dgam, dbet, jnp.zeros((6, D), F32)], axis=0)
    for k in range(1, 8):
        small(ex_gb, gb_s, gb_r, k).start()

    def phase8(t):
        y_v[t] = (x_v[t].astype(F32) + mm(ot[t].T, wo_ref[...])).astype(BF16)

    for t in range(nb):
        phase8(t)
        go_on(8, t, 1)

    for c in range(4):
        for h in range(PIECES[c]):
            stage_c(c, h).wait_recv()
        both = sb[c] + rc[c]
        if c == 0:
            gwo_ref[...] = both
        else:
            col = {1: 2 * D, 2: 0, 3: D}[c]
            gwqkv_ref[:, col : col + D] = both
    t_copy.wait_recv()
    gtau_ref[...] = (ex_t[0] + ex_t[1])[0, 0:H]
    for k in range(1, 8):
        small(ex_gb, gb_s, gb_r, k).wait_recv()
    gb = ((ex_gb[0] + ex_gb[1]) + (ex_gb[2] + ex_gb[3])) + ((ex_gb[4] + ex_gb[5]) + (ex_gb[6] + ex_gb[7]))
    ggam_ref[...] = gb[0]
    gbet_ref[...] = gb[1]

    for k in range(1, 4):
        small(ex_a, exa_s, exa_r, k).wait_send()
    for c in range(4):
        for xx in range(2):
            stage_a(c, xx).wait_send()
        for h in range(PIECES[c]):
            stage_b(c, h).wait_send()
            stage_c(c, h).wait_send()
    g_core.wait_send()
    g_chip.wait_send()
    t_copy.wait_send()
    for k in range(1, 8):
        small(ex_gb, gb_s, gb_r, k).wait_send()


def store_kernel(*refs):
    sem = refs[14]
    copies = []
    for i in range(7):
        src, dst = refs[i], refs[7 + i]
        for at in range(src.shape[0]) if i < 2 else [None]:
            pair = (src, dst) if at is None else (src.at[at], dst.at[at])
            copies.append(pltpu.make_async_copy(*pair, sem.at[len(copies)]))
    for copy in copies:
        copy.start()
    for copy in copies:
        copy.wait()


def solution(mesh):
    act_spec = P(("data", "img"), "seq", None)
    row_spec = P(("data", "seq"), None)
    in_specs = (act_spec, act_spec, P(), P(), P(), P(), P())
    out_specs = (act_spec, act_spec, row_spec, row_spec, P("data"), P("data"), P("data"))

    def local_block(x_in, grad_y, ln_gamma, ln_beta, w_qkv, w_out, head_temp):
        n_tok = x_in.shape[1]
        nb = n_tok // TB
        hbm = pl.BlockSpec(memory_space=pl.ANY)
        vmem = pl.BlockSpec(memory_space=pltpu.VMEM)
        dma = pltpu.SemaphoreType.DMA
        outs = pl.pallas_call(
            functools.partial(kernel, nb),
            out_shape=(
                pltpu.VMEM((nb, TB, D), BF16),
                pltpu.VMEM((nb, TB, D), BF16),
                pltpu.VMEM((ROWS, 3 * D), F32),
                pltpu.VMEM((ROWS, D), F32),
                pltpu.VMEM((D,), F32),
                pltpu.VMEM((D,), F32),
                pltpu.VMEM((H,), F32),
            ),
            in_specs=[hbm] * 7,
            out_specs=(vmem,) * 7,
            scratch_shapes=[
                pltpu.VMEM((nb, TB, D), BF16),
                pltpu.VMEM((nb, TB, D), BF16),
                pltpu.VMEM((nb, D, TB), BF16),
                pltpu.VMEM((nb, 3 * D, TB), BF16),
                pltpu.VMEM((nb, D, TB), BF16),
                pltpu.VMEM((nb, D, TB), BF16),
                pltpu.VMEM((nb, TB, 128), F32),
                pltpu.VMEM((nb, TB, 128), F32),
                pltpu.VMEM((3 * D, D), BF16),
                pltpu.VMEM((D,), F32),
                pltpu.VMEM((D,), F32),
                pltpu.VMEM((D, 3 * D), BF16),
                pltpu.VMEM((D, D), BF16),
                pltpu.SMEM((H,), F32),
                pltpu.VMEM((SPLIT, 256), F32),
                pltpu.VMEM((D - SPLIT, 256), F32),
                pltpu.VMEM((D, 128), F32),
                pltpu.VMEM((D, 128), F32),
                pltpu.VMEM((2, C + 8, D), F32),
                pltpu.VMEM((2, C + 8, D), F32),
                pltpu.VMEM((4, C, D), F32),
                pltpu.VMEM((H, C, D), F32),
                pltpu.VMEM((D, D), BF16),
                pltpu.VMEM((D, D), BF16),
                pltpu.VMEM((D, D), BF16),
                pltpu.VMEM((D, D), BF16),
                pltpu.VMEM((D, 128), F32),
                pltpu.VMEM((D, 128), F32),
                pltpu.VMEM((4, D, D), F32),
                pltpu.VMEM((4, 2, ROWS, D), F32),
                pltpu.VMEM((4, 2, ROWS, D), F32),
                pltpu.VMEM((4, ROWS, D), F32),
                pltpu.VMEM((4, ROWS, D), F32),
                pltpu.VMEM((4, ROWS, D), F32),
                pltpu.VMEM((2, 8, D), F32),
                pltpu.VMEM((8, 8, D), F32),
                pltpu.VMEM((2, 8, 128), F32),
                dma((nb,)), dma((nb,)), dma((5,)),
                dma((2,)), dma((2,)), dma((4,)), dma((4,)),
                dma((4, 2)), dma((4, 2)), dma((4, max(PIECES))), dma((4, max(PIECES))), dma((4, max(PIECES))), dma((4, max(PIECES))),
                dma((8,)), dma((8,)), dma, dma,
            ],
            compiler_params=pltpu.CompilerParams(
                collective_id=0, has_side_effects=True, vmem_limit_bytes=52000000
            ),
            name="xca_block",
        )(
            x_in.reshape(nb, TB, D),
            grad_y.reshape(nb, TB, D),
            ln_gamma,
            ln_beta,
            w_qkv,
            w_out,
            head_temp,
        )
        outs = pl.pallas_call(
            store_kernel,
            out_shape=(
                jax.ShapeDtypeStruct((nb, TB, D), BF16),
                jax.ShapeDtypeStruct((nb, TB, D), BF16),
                jax.ShapeDtypeStruct((ROWS, 3 * D), F32),
                jax.ShapeDtypeStruct((ROWS, D), F32),
                jax.ShapeDtypeStruct((D,), F32),
                jax.ShapeDtypeStruct((D,), F32),
                jax.ShapeDtypeStruct((H,), F32),
            ),
            in_specs=[hbm] * 7,
            out_specs=(hbm,) * 7,
            scratch_shapes=[dma((2 * nb + 5,))],
            compiler_params=pltpu.CompilerParams(vmem_limit_bytes=4 * 2**20),
            name="xca_store",
        )(*outs)
        y, dx, gwqkv, gwo, ggam, gbet, gtau = outs
        return y.reshape(1, n_tok, D), dx.reshape(1, n_tok, D), gwqkv, gwo, ggam, gbet, gtau

    return jax.shard_map(local_block, mesh=mesh, in_specs=in_specs, out_specs=out_specs, check_vma=False)
```

```python
import functools

import jax
import jax.numpy as jnp
from jax import lax
from jax.experimental import pallas as pl
from jax.experimental.pallas import tpu as pltpu
from jax.sharding import PartitionSpec as P

LN_EPS = 1e-6
MESH = pl.DeviceIdType.MESH
F32 = jnp.float32
BF16 = jnp.bfloat16

D = 384
H = 8
C = 48
SPLIT = 240
OFF = 128
ROWS = 96
TB = 1024
PIECES = (2, 1, 1, 2)
STEPS = {
    (4, 3): [("b", 0, 0)],
    (5, 2): [("b", 1, 0), ("c", 0, 0)],
    (6, 2): [("b", 2, 0), ("c", 0, 1)],
    (7, 0, 1): [("b", 3, 0), ("c", 1, 0)],
    (7, 2, 1): [("c", 2, 0)],
    (7, 3, 1): [("c", 3, 0), ("c", 3, 1)],
}


def mm(a, b):
    return jnp.dot(a, b, preferred_element_type=F32)


def mm_nt(a, b):
    return lax.dot_general(a, b, (((1,), (1,)), ((), ())), preferred_element_type=F32)


def col_mask(h):
    col = lax.broadcasted_iota(jnp.int32, (C, D), 1)
    return (col >= C * h) & (col < C * h + C)


def to_column(row, h):
    col = lax.broadcasted_iota(jnp.int32, (C, D), 1)
    line = lax.broadcasted_iota(jnp.int32, (C, D), 0)
    return jnp.sum(jnp.where(col == line + C * h, row, 0.0), axis=1, keepdims=True)


def to_row(column, h):
    col = lax.broadcasted_iota(jnp.int32, (C, D), 1)
    line = lax.broadcasted_iota(jnp.int32, (C, D), 0)
    return jnp.sum(jnp.where(col == line + C * h, column, 0.0), axis=0, keepdims=True)


def pack(lo, hi):
    p_lo = jnp.zeros((C, 256), F32)
    p_hi = jnp.zeros((C, 256), F32)
    for h in range(5):
        p_lo += jnp.where(col_mask(h)[:, 0:256], lo[C * h : C * h + C, :], 0.0)
    for h in range(5, H):
        r = C * h - SPLIT
        p_hi += jnp.where(col_mask(h)[:, OFF:D], hi[r : r + C, :], 0.0)
    return jnp.concatenate([p_lo[:, 0:128], p_lo[:, 128:256] + p_hi[:, 0:128], p_hi[:, 128:256]], axis=1)


def block_mm(w, act):
    lo = mm(w[0:SPLIT, 0:256], act[0:256, :])
    hi = mm(w[SPLIT:D, OFF:D], act[OFF:D, :])
    return lo, hi


def kernel(
    nb,
    x_hbm, dy_hbm, gamma_hbm, beta_hbm, wqkv_hbm, wo_hbm, tau_hbm,
    y_v, dx_v, gwqkv_ref, gwo_ref, ggam_ref, gbet_ref, gtau_ref,
    x_v, dy_v, ut, qkvt, dot_v, ot, mean_v, rstd_v, wqkvt,
    gamma_ref, beta_ref, wqkv_ref, wo_ref, tau_ref,
    g_lo, g_hi, sq_acc, sk_acc, ex_g, ex_h, ex_a, a_f, a_b, a_bt, dg_b, dg_bt, dsq_v, dsk_v,
    pw, ra, sa, rb, sb, rc, gb_acc, ex_gb, ex_t,
    x_sem, dy_sem, in_sem,
    exg_s, exg_r, exa_s, exa_r, a_s, a_r, b_s, b_r, c_s, c_r, gb_s, gb_r, t_s, t_r,
):
    data = lax.axis_index("data")
    img = lax.axis_index("img")
    seq = lax.axis_index("seq")
    xc = seq // 2
    core = seq % 2

    def dev(k):
        i = 1 - img if k & 4 else img
        xx = 1 - xc if k & 2 else xc
        cc = 1 - core if k & 1 else core
        return (data, i, xx * 2 + cc)

    barrier = pltpu.get_barrier_semaphore()
    for k in range(1, 8):
        pl.semaphore_signal(barrier, inc=1, device_id=dev(k), device_id_type=MESH)

    def x_in(t):
        return pltpu.make_async_copy(x_hbm.at[t], x_v.at[t], x_sem.at[t])

    def dy_in(t):
        return pltpu.make_async_copy(dy_hbm.at[t], dy_v.at[t], dy_sem.at[t])

    def weight_in(i):
        pairs = ((wqkv_hbm, wqkv_ref), (gamma_hbm, gamma_ref), (beta_hbm, beta_ref), (wo_hbm, wo_ref), (tau_hbm, tau_ref))
        return pltpu.make_async_copy(*pairs[i], in_sem.at[i])

    weight_in(0).start()
    x_in(0).start()
    for i in range(1, 5):
        weight_in(i).start()

    def remote(src, dst, s, r, k):
        return pltpu.make_async_remote_copy(
            src_ref=src, dst_ref=dst, send_sem=s, recv_sem=r, device_id=dev(k), device_id_type=MESH
        )

    def small(buf, s, r, k):
        return remote(buf.at[0], buf.at[k], s.at[k], r.at[k], k)

    def stage_a(c, xx):
        rows = pl.ds(pl.multiple_of(ROWS * (2 * xx + 1 - core), 8), ROWS)
        return remote(pw.at[c, rows, :], ra.at[c, xx], a_s.at[c, xx], a_r.at[c, xx], 1)

    def part(c, h):
        return pl.ds(h * (ROWS // PIECES[c]), ROWS // PIECES[c])

    def stage_b(c, h):
        return remote(sa.at[c, 1 - xc, part(c, h)], rb.at[c, part(c, h)], b_s.at[c, h], b_r.at[c, h], 2)

    def stage_c(c, h):
        return remote(sb.at[c, part(c, h)], rc.at[c, part(c, h)], c_s.at[c, h], c_r.at[c, h], 4)

    def start_a(c):
        for xx in range(2):
            stage_a(c, xx).start()

    def start_b(c):
        for xx in range(2):
            stage_a(c, xx).wait_recv()
            rows = pl.ds(pl.multiple_of(ROWS * (2 * xx + core), 8), ROWS)
            sa[c, xx] = pw[c, rows, :] + ra[c, xx]
        for h in range(PIECES[c]):
            stage_b(c, h).start()

    def start_c(c, h):
        stage_b(c, h).wait_recv()
        sb[c, part(c, h)] = sa[c, xc, part(c, h)] + rb[c, part(c, h)]
        stage_c(c, h).start()

    def total(product):
        out = product(0)
        for t in range(1, nb):
            out = out + product(t)
        return out

    def go_on(*at):
        for stage, c, h in STEPS.get(at, ()):
            if stage == "b":
                start_b(c)
            else:
                start_c(c, h)

    for ref in (g_lo, g_hi, sq_acc, sk_acc, gb_acc):
        ref[...] = jnp.zeros_like(ref)
    for i in range(3):
        weight_in(i).wait()
    wqkvt[...] = wqkv_ref[...].T
    x_in(0).wait()
    for t in range(1, nb):
        x_in(t).start()
    gamma = gamma_ref[...].reshape(1, D)
    beta = beta_ref[...].reshape(1, D)

    def lane_fold(a):
        out = a[:, 0:128]
        for i in range(1, TB // 128):
            out = out + a[:, 128 * i : 128 * i + 128]
        return out

    def phase1(t):
        x = x_v[t].astype(F32)
        mean = jnp.mean(x, axis=-1, keepdims=True)
        cen = x - mean
        var = jnp.mean(cen * cen, axis=-1, keepdims=True)
        rstd = lax.rsqrt(var + LN_EPS)
        mean_v[t] = jnp.broadcast_to(mean, (TB, 128))
        rstd_v[t] = jnp.broadcast_to(rstd, (TB, 128))
        u = (cen * rstd * gamma + beta).astype(BF16)
        u_t = u.T
        ut[t] = u_t
        qk = mm(wqkvt[0 : 2 * D, :], u_t).astype(BF16)
        qkvt[t, 0 : 2 * D, :] = qk
        q = qk[0:D, :]
        k = qk[D : 2 * D, :]
        g_lo[...] += mm_nt(q[0:SPLIT, :], k[0:256, :])
        g_hi[...] += mm_nt(q[SPLIT:D, :], k[OFF:D, :])
        qf = q.astype(F32)
        kf = k.astype(F32)
        sq_acc[...] += lane_fold(qf * qf)
        sk_acc[...] += lane_fold(kf * kf)

    for t in range(nb):
        if t == 1:
            for n in range(1, nb):
                x_in(n).wait()
            for n in range(nb):
                dy_in(n).start()
            for i in range(3, 5):
                weight_in(i).wait()
        phase1(t)

    ex_g[0, 0:C, :] = pack(g_lo[...], g_hi[...])
    sq_row = jnp.zeros((1, D), F32)
    sk_row = jnp.zeros((1, D), F32)
    for h in range(H):
        rows = slice(C * h, C * h + C)
        sq_row += to_row(jnp.sum(sq_acc[rows, :], axis=1, keepdims=True), h)
        sk_row += to_row(jnp.sum(sk_acc[rows, :], axis=1, keepdims=True), h)
    ex_g[0, C : C + 8, :] = jnp.concatenate([sq_row, sk_row, jnp.zeros((6, D), F32)], axis=0)
    pl.semaphore_wait(barrier, 7)
    g_core = remote(ex_g.at[0], ex_g.at[1], exg_s.at[0], exg_r.at[0], 1)
    g_chip = remote(ex_h.at[0], ex_h.at[1], exg_s.at[1], exg_r.at[1], 2)
    g_core.start()
    for t in range(nb):
        dy_in(t).wait()

    def gram_step():
        g_core.wait_recv()
        ex_h[0] = ex_g[0] + ex_g[1]
        g_chip.start()

    g_lo[...] = jnp.zeros_like(g_lo)
    g_hi[...] = jnp.zeros_like(g_hi)

    def phase2(t):
        v = mm(wqkvt[2 * D : 3 * D, :], ut[t]).astype(BF16)
        qkvt[t, 2 * D : 3 * D, :] = v
        do = mm_nt(wo_ref[...], dy_v[t]).astype(BF16)
        dot_v[t] = do
        g_lo[...] += mm_nt(do[0:SPLIT, :], v[0:256, :])
        g_hi[...] += mm_nt(do[SPLIT:D, :], v[OFF:D, :])

    for t in range(nb):
        phase2(t)
        if t == 0:
            gram_step()
    ex_a[0] = pack(g_lo[...], g_hi[...])
    for k in range(1, 4):
        small(ex_a, exa_s, exa_r, k).start()

    g_chip.wait_recv()
    gram_all = ex_h[0] + ex_h[1]
    gram = gram_all[0:C, :]
    sq_row = gram_all[C : C + 1, :]
    sk_row = gram_all[C + 1 : C + 2, :]
    rk = lax.rsqrt(sk_row)
    for h in range(H):
        m = col_mask(h)
        rq = lax.rsqrt(to_column(sq_row, h))
        z = jnp.where(m, gram * (tau_ref[h] * rq * rk), -jnp.inf)
        e = jnp.exp(z - jnp.max(z, axis=1, keepdims=True))
        a = e / jnp.sum(e, axis=1, keepdims=True)
        a_f[h] = a
        a_b[C * h : C * h + C, :] = a.astype(BF16)
    a_bt[...] = a_b[...].T

    def phase3(t):
        o_lo, o_hi = block_mm(a_b[...], qkvt[t, 2 * D : 3 * D, :])
        ot[t, 0:SPLIT, :] = o_lo.astype(BF16)
        ot[t, SPLIT:D, :] = o_hi.astype(BF16)

    for t in range(nb):
        phase3(t)
    pw[0] = total(lambda t: mm(ot[t], dy_v[t]))
    start_a(0)

    def phase4(t):
        dv_lo, dv_hi = block_mm(a_bt[...], dot_v[t])
        qkvt[t, 2 * D : 2 * D + SPLIT, :] = dv_lo.astype(BF16)
        qkvt[t, 2 * D + SPLIT : 3 * D, :] = dv_hi.astype(BF16)

    for t in range(nb):
        phase4(t)
    go_on(4, 0)
    pw[1, :, 0:256] = total(lambda t: mm_nt(ut[t], qkvt[t, 2 * D : 2 * D + 256, :]))
    go_on(4, 1)
    pw[1, :, 256:D] = total(lambda t: mm_nt(ut[t], qkvt[t, 2 * D + 256 : 3 * D, :]))
    go_on(4, 2)
    start_a(1)

    for k in range(1, 4):
        small(ex_a, exa_s, exa_r, k).wait_recv()
    go_on(4, 3)
    d_attn = (ex_a[0] + ex_a[1]) + (ex_a[2] + ex_a[3])
    drk = jnp.zeros((1, D), F32)
    lane = lax.broadcasted_iota(jnp.int32, (8, 128), 1)
    dtau = jnp.zeros((8, 128), F32)
    for h in range(H):
        m = col_mask(h)
        tau = tau_ref[h]
        sq = to_column(sq_row, h)
        rq = lax.rsqrt(sq)
        a = a_f[h]
        da = jnp.where(m, d_attn, 0.0)
        dz = a * (da - jnp.sum(da * a, axis=1, keepdims=True))
        dg_b[C * h : C * h + C, :] = jnp.where(m, dz * (tau * rq * rk), 0.0).astype(BF16)
        w = dz * gram
        wrk = jnp.sum(jnp.where(m, w * rk, 0.0), axis=1, keepdims=True)
        dsq = (tau * wrk) * (-0.5 * (rq / sq))
        dsq_v[C * h : C * h + C, :] = jnp.broadcast_to(2.0 * dsq, (C, 128))
        drk += jnp.sum(jnp.where(m, w * (tau * rq), 0.0), axis=0, keepdims=True)
        dtau += jnp.where(lane == h, jnp.sum(wrk * rq), 0.0)
    dsk = drk * (-0.5 * (rk / sk_row))
    for h in range(H):
        dsk_v[C * h : C * h + C, :] = jnp.broadcast_to(2.0 * to_column(dsk, h), (C, 128))
    dg_bt[...] = dg_b[...].T
    ex_t[0] = dtau
    t_copy = remote(ex_t.at[0], ex_t.at[1], t_s, t_r, 4)
    t_copy.start()

    def phase5(t):
        dq_lo, dq_hi = block_mm(dg_b[...], qkvt[t, D : 2 * D, :])
        qf = qkvt[t, 0:D, :].astype(F32)
        ds = dsq_v[:, 0:1]
        dot_v[t, 0:SPLIT, :] = (dq_lo + ds[0:SPLIT] * qf[0:SPLIT]).astype(BF16)
        dot_v[t, SPLIT:D, :] = (dq_hi + ds[SPLIT:D] * qf[SPLIT:D]).astype(BF16)

    for t in range(nb):
        phase5(t)
    go_on(5, 0)
    pw[2, :, 0:256] = total(lambda t: mm_nt(ut[t], dot_v[t, 0:256, :]))
    go_on(5, 1)
    pw[2, :, 256:D] = total(lambda t: mm_nt(ut[t], dot_v[t, 256:D, :]))
    go_on(5, 2)
    start_a(2)

    def phase6(t):
        dk_lo, dk_hi = block_mm(dg_bt[...], qkvt[t, 0:D, :])
        kf = qkvt[t, D : 2 * D, :].astype(F32)
        ds = dsk_v[:, 0:1]
        qkvt[t, D : D + SPLIT, :] = (dk_lo + ds[0:SPLIT] * kf[0:SPLIT]).astype(BF16)
        qkvt[t, D + SPLIT : 2 * D, :] = (dk_hi + ds[SPLIT:D] * kf[SPLIT:D]).astype(BF16)

    for t in range(nb):
        phase6(t)
    go_on(6, 0)
    pw[3, :, 0:256] = total(lambda t: mm_nt(ut[t], qkvt[t, D : D + 256, :]))
    go_on(6, 1)
    pw[3, :, 256:D] = total(lambda t: mm_nt(ut[t], qkvt[t, D + 256 : 2 * D, :]))
    go_on(6, 2)
    start_a(3)

    def phase7(t, half):
        rows = slice(half * (TB // 2), (half + 1) * (TB // 2))
        du_t = mm(wqkv_ref[:, 0:D], dot_v[t, :, rows]) + mm(wqkv_ref[:, D : 3 * D], qkvt[t, D : 3 * D, rows])
        du = du_t.astype(BF16).T.astype(F32)
        rstd = rstd_v[t, rows, 0:1]
        xhat = (x_v[t, rows].astype(F32) - mean_v[t, rows, 0:1]) * rstd
        g = du * gamma
        m1 = jnp.mean(g, axis=-1, keepdims=True)
        m2 = jnp.mean(g * xhat, axis=-1, keepdims=True)
        dx = rstd * (g - m1 - xhat * m2)
        dx_v[t, rows] = (dy_v[t, rows].astype(F32) + dx).astype(BF16)
        gb_acc[0] += jnp.sum((du * xhat).reshape(TB // 16, 8, D), axis=0)
        gb_acc[1] += jnp.sum(du.reshape(TB // 16, 8, D), axis=0)

    for t in range(nb):
        for half in range(2):
            phase7(t, half)
            go_on(7, t, half)

    dgam = jnp.sum(gb_acc[0], axis=0, keepdims=True)
    dbet = jnp.sum(gb_acc[1], axis=0, keepdims=True)
    ex_gb[0] = jnp.concatenate([dgam, dbet, jnp.zeros((6, D), F32)], axis=0)
    for k in range(1, 8):
        small(ex_gb, gb_s, gb_r, k).start()

    def phase8(t):
        y_v[t] = (x_v[t].astype(F32) + mm(ot[t].T, wo_ref[...])).astype(BF16)

    for t in range(nb):
        phase8(t)
        go_on(8, t, 1)

    for c in range(4):
        for h in range(PIECES[c]):
            stage_c(c, h).wait_recv()
        both = sb[c] + rc[c]
        if c == 0:
            gwo_ref[...] = both
        else:
            col = {1: 2 * D, 2: 0, 3: D}[c]
            gwqkv_ref[:, col : col + D] = both
    t_copy.wait_recv()
    gtau_ref[...] = (ex_t[0] + ex_t[1])[0, 0:H]
    for k in range(1, 8):
        small(ex_gb, gb_s, gb_r, k).wait_recv()
    gb = ((ex_gb[0] + ex_gb[1]) + (ex_gb[2] + ex_gb[3])) + ((ex_gb[4] + ex_gb[5]) + (ex_gb[6] + ex_gb[7]))
    ggam_ref[...] = gb[0]
    gbet_ref[...] = gb[1]

    for k in range(1, 4):
        small(ex_a, exa_s, exa_r, k).wait_send()
    for c in range(4):
        for xx in range(2):
            stage_a(c, xx).wait_send()
        for h in range(PIECES[c]):
            stage_b(c, h).wait_send()
            stage_c(c, h).wait_send()
    g_core.wait_send()
    g_chip.wait_send()
    t_copy.wait_send()
    for k in range(1, 8):
        small(ex_gb, gb_s, gb_r, k).wait_send()


def store_kernel(*refs):
    sem = refs[14]
    copies = []
    for i in range(7):
        src, dst = refs[i], refs[7 + i]
        for at in range(src.shape[0]) if i < 2 else [None]:
            pair = (src, dst) if at is None else (src.at[at], dst.at[at])
            copies.append(pltpu.make_async_copy(*pair, sem.at[len(copies)]))
    for copy in copies:
        copy.start()
    for copy in copies:
        copy.wait()


def solution(mesh):
    act_spec = P(("data", "img"), "seq", None)
    row_spec = P(("data", "seq"), None)
    in_specs = (act_spec, act_spec, P(), P(), P(), P(), P())
    out_specs = (act_spec, act_spec, row_spec, row_spec, P("data"), P("data"), P("data"))

    def local_block(x_in, grad_y, ln_gamma, ln_beta, w_qkv, w_out, head_temp):
        n_tok = x_in.shape[1]
        nb = n_tok // TB
        hbm = pl.BlockSpec(memory_space=pl.ANY)
        vmem = pl.BlockSpec(memory_space=pltpu.VMEM)
        dma = pltpu.SemaphoreType.DMA
        outs = pl.pallas_call(
            functools.partial(kernel, nb),
            out_shape=(
                pltpu.VMEM((nb, TB, D), BF16),
                pltpu.VMEM((nb, TB, D), BF16),
                pltpu.VMEM((ROWS, 3 * D), F32),
                pltpu.VMEM((ROWS, D), F32),
                pltpu.VMEM((D,), F32),
                pltpu.VMEM((D,), F32),
                pltpu.VMEM((H,), F32),
            ),
            in_specs=[hbm] * 7,
            out_specs=(vmem,) * 7,
            scratch_shapes=[
                pltpu.VMEM((nb, TB, D), BF16),
                pltpu.VMEM((nb, TB, D), BF16),
                pltpu.VMEM((nb, D, TB), BF16),
                pltpu.VMEM((nb, 3 * D, TB), BF16),
                pltpu.VMEM((nb, D, TB), BF16),
                pltpu.VMEM((nb, D, TB), BF16),
                pltpu.VMEM((nb, TB, 128), F32),
                pltpu.VMEM((nb, TB, 128), F32),
                pltpu.VMEM((3 * D, D), BF16),
                pltpu.VMEM((D,), F32),
                pltpu.VMEM((D,), F32),
                pltpu.VMEM((D, 3 * D), BF16),
                pltpu.VMEM((D, D), BF16),
                pltpu.SMEM((H,), F32),
                pltpu.VMEM((SPLIT, 256), F32),
                pltpu.VMEM((D - SPLIT, 256), F32),
                pltpu.VMEM((D, 128), F32),
                pltpu.VMEM((D, 128), F32),
                pltpu.VMEM((2, C + 8, D), F32),
                pltpu.VMEM((2, C + 8, D), F32),
                pltpu.VMEM((4, C, D), F32),
                pltpu.VMEM((H, C, D), F32),
                pltpu.VMEM((D, D), BF16),
                pltpu.VMEM((D, D), BF16),
                pltpu.VMEM((D, D), BF16),
                pltpu.VMEM((D, D), BF16),
                pltpu.VMEM((D, 128), F32),
                pltpu.VMEM((D, 128), F32),
                pltpu.VMEM((4, D, D), F32),
                pltpu.VMEM((4, 2, ROWS, D), F32),
                pltpu.VMEM((4, 2, ROWS, D), F32),
                pltpu.VMEM((4, ROWS, D), F32),
                pltpu.VMEM((4, ROWS, D), F32),
                pltpu.VMEM((4, ROWS, D), F32),
                pltpu.VMEM((2, 8, D), F32),
                pltpu.VMEM((8, 8, D), F32),
                pltpu.VMEM((2, 8, 128), F32),
                dma((nb,)), dma((nb,)), dma((5,)),
                dma((2,)), dma((2,)), dma((4,)), dma((4,)),
                dma((4, 2)), dma((4, 2)), dma((4, max(PIECES))), dma((4, max(PIECES))), dma((4, max(PIECES))), dma((4, max(PIECES))),
                dma((8,)), dma((8,)), dma, dma,
            ],
            compiler_params=pltpu.CompilerParams(
                collective_id=0, has_side_effects=True, vmem_limit_bytes=52000000
            ),
            name="xca_block",
        )(
            x_in.reshape(nb, TB, D),
            grad_y.reshape(nb, TB, D),
            ln_gamma,
            ln_beta,
            w_qkv,
            w_out,
            head_temp,
        )
        outs = pl.pallas_call(
            store_kernel,
            out_shape=(
                jax.ShapeDtypeStruct((nb, TB, D), BF16),
                jax.ShapeDtypeStruct((nb, TB, D), BF16),
                jax.ShapeDtypeStruct((ROWS, 3 * D), F32),
                jax.ShapeDtypeStruct((ROWS, D), F32),
                jax.ShapeDtypeStruct((D,), F32),
                jax.ShapeDtypeStruct((D,), F32),
                jax.ShapeDtypeStruct((H,), F32),
            ),
            in_specs=[hbm] * 7,
            out_specs=(hbm,) * 7,
            scratch_shapes=[dma((2 * nb + 5,))],
            compiler_params=pltpu.CompilerParams(vmem_limit_bytes=4 * 2**20),
            name="xca_store",
        )(*outs)
        y, dx, gwqkv, gwo, ggam, gbet, gtau = outs
        return y.reshape(1, n_tok, D), dx.reshape(1, n_tok, D), gwqkv, gwo, ggam, gbet, gtau

    return jax.shard_map(local_block, mesh=mesh, in_specs=in_specs, out_specs=out_specs, check_vma=False)
```

```python
import functools

import jax
import jax.numpy as jnp
from jax import lax
from jax.experimental import pallas as pl
from jax.experimental.pallas import tpu as pltpu
from jax.sharding import PartitionSpec as P

LN_EPS = 1e-6
MESH = pl.DeviceIdType.MESH
F32 = jnp.float32
BF16 = jnp.bfloat16

D = 384
H = 8
C = 48
SPLIT = 240
OFF = 128
ROWS = 96
TB = 1024
PIECES = (3, 1, 1, 2)
STEPS = {
    (4, 3): [("b", 0, 0)],
    (5, 2): [("b", 1, 0), ("c", 0, 0)],
    (6, 2): [("b", 2, 0), ("c", 0, 1), ("c", 0, 2)],
    (7, 0, 1): [("b", 3, 0), ("c", 1, 0)],
    (7, 2, 1): [("c", 2, 0)],
    (7, 3, 1): [("c", 3, 0), ("c", 3, 1)],
}


def mm(a, b):
    return jnp.dot(a, b, preferred_element_type=F32)


def mm_nt(a, b):
    return lax.dot_general(a, b, (((1,), (1,)), ((), ())), preferred_element_type=F32)


def col_mask(h):
    col = lax.broadcasted_iota(jnp.int32, (C, D), 1)
    return (col >= C * h) & (col < C * h + C)


def to_column(row, h):
    col = lax.broadcasted_iota(jnp.int32, (C, D), 1)
    line = lax.broadcasted_iota(jnp.int32, (C, D), 0)
    return jnp.sum(jnp.where(col == line + C * h, row, 0.0), axis=1, keepdims=True)


def to_row(column, h):
    col = lax.broadcasted_iota(jnp.int32, (C, D), 1)
    line = lax.broadcasted_iota(jnp.int32, (C, D), 0)
    return jnp.sum(jnp.where(col == line + C * h, column, 0.0), axis=0, keepdims=True)


def pack(lo, hi):
    p_lo = jnp.zeros((C, 256), F32)
    p_hi = jnp.zeros((C, 256), F32)
    for h in range(5):
        p_lo += jnp.where(col_mask(h)[:, 0:256], lo[C * h : C * h + C, :], 0.0)
    for h in range(5, H):
        r = C * h - SPLIT
        p_hi += jnp.where(col_mask(h)[:, OFF:D], hi[r : r + C, :], 0.0)
    return jnp.concatenate([p_lo[:, 0:128], p_lo[:, 128:256] + p_hi[:, 0:128], p_hi[:, 128:256]], axis=1)


def block_mm(w, act):
    lo = mm(w[0:SPLIT, 0:256], act[0:256, :])
    hi = mm(w[SPLIT:D, OFF:D], act[OFF:D, :])
    return lo, hi


def kernel(
    nb,
    x_hbm, dy_hbm, gamma_hbm, beta_hbm, wqkv_hbm, wo_hbm, tau_hbm,
    y_v, dx_v, gwqkv_ref, gwo_ref, ggam_ref, gbet_ref, gtau_ref,
    x_v, dy_v, ut, qkvt, dot_v, ot, mean_v, rstd_v, wqkvt,
    gamma_ref, beta_ref, wqkv_ref, wo_ref, tau_ref,
    g_lo, g_hi, sq_acc, sk_acc, ex_g, ex_h, ex_a, a_f, a_b, a_bt, dg_b, dg_bt, dsq_v, dsk_v,
    pw, ra, sa, rb, sb, rc, gb_acc, ex_gb, ex_t,
    x_sem, dy_sem, in_sem,
    exg_s, exg_r, exa_s, exa_r, a_s, a_r, b_s, b_r, c_s, c_r, gb_s, gb_r, t_s, t_r,
):
    data = lax.axis_index("data")
    img = lax.axis_index("img")
    seq = lax.axis_index("seq")
    xc = seq // 2
    core = seq % 2

    def dev(k):
        i = 1 - img if k & 4 else img
        xx = 1 - xc if k & 2 else xc
        cc = 1 - core if k & 1 else core
        return (data, i, xx * 2 + cc)

    barrier = pltpu.get_barrier_semaphore()
    for k in range(1, 8):
        pl.semaphore_signal(barrier, inc=1, device_id=dev(k), device_id_type=MESH)

    def x_in(t):
        return pltpu.make_async_copy(x_hbm.at[t], x_v.at[t], x_sem.at[t])

    def dy_in(t):
        return pltpu.make_async_copy(dy_hbm.at[t], dy_v.at[t], dy_sem.at[t])

    def weight_in(i):
        pairs = ((wqkv_hbm, wqkv_ref), (gamma_hbm, gamma_ref), (beta_hbm, beta_ref), (wo_hbm, wo_ref), (tau_hbm, tau_ref))
        return pltpu.make_async_copy(*pairs[i], in_sem.at[i])

    weight_in(0).start()
    x_in(0).start()
    for i in range(1, 5):
        weight_in(i).start()

    def remote(src, dst, s, r, k):
        return pltpu.make_async_remote_copy(
            src_ref=src, dst_ref=dst, send_sem=s, recv_sem=r, device_id=dev(k), device_id_type=MESH
        )

    def small(buf, s, r, k):
        return remote(buf.at[0], buf.at[k], s.at[k], r.at[k], k)

    def stage_a(c, xx):
        rows = pl.ds(pl.multiple_of(ROWS * (2 * xx + 1 - core), 8), ROWS)
        return remote(pw.at[c, rows, :], ra.at[c, xx], a_s.at[c, xx], a_r.at[c, xx], 1)

    def part(c, h):
        return pl.ds(h * (ROWS // PIECES[c]), ROWS // PIECES[c])

    def stage_b(c, h):
        return remote(sa.at[c, 1 - xc, part(c, h)], rb.at[c, part(c, h)], b_s.at[c, h], b_r.at[c, h], 2)

    def stage_c(c, h):
        return remote(sb.at[c, part(c, h)], rc.at[c, part(c, h)], c_s.at[c, h], c_r.at[c, h], 4)

    def start_a(c):
        for xx in range(2):
            stage_a(c, xx).start()

    def start_b(c):
        for xx in range(2):
            stage_a(c, xx).wait_recv()
            rows = pl.ds(pl.multiple_of(ROWS * (2 * xx + core), 8), ROWS)
            sa[c, xx] = pw[c, rows, :] + ra[c, xx]
        for h in range(PIECES[c]):
            stage_b(c, h).start()

    def start_c(c, h):
        stage_b(c, h).wait_recv()
        sb[c, part(c, h)] = sa[c, xc, part(c, h)] + rb[c, part(c, h)]
        stage_c(c, h).start()

    def total(product):
        out = product(0)
        for t in range(1, nb):
            out = out + product(t)
        return out

    def go_on(*at):
        for stage, c, h in STEPS.get(at, ()):
            if stage == "b":
                start_b(c)
            else:
                start_c(c, h)

    for ref in (g_lo, g_hi, sq_acc, sk_acc, gb_acc):
        ref[...] = jnp.zeros_like(ref)
    for i in range(3):
        weight_in(i).wait()
    wqkvt[...] = wqkv_ref[...].T
    x_in(0).wait()
    for t in range(1, nb):
        x_in(t).start()
    gamma = gamma_ref[...].reshape(1, D)
    beta = beta_ref[...].reshape(1, D)

    def lane_fold(a):
        out = a[:, 0:128]
        for i in range(1, TB // 128):
            out = out + a[:, 128 * i : 128 * i + 128]
        return out

    def phase1(t):
        x = x_v[t].astype(F32)
        mean = jnp.mean(x, axis=-1, keepdims=True)
        cen = x - mean
        var = jnp.mean(cen * cen, axis=-1, keepdims=True)
        rstd = lax.rsqrt(var + LN_EPS)
        mean_v[t] = jnp.broadcast_to(mean, (TB, 128))
        rstd_v[t] = jnp.broadcast_to(rstd, (TB, 128))
        u = (cen * rstd * gamma + beta).astype(BF16)
        u_t = u.T
        ut[t] = u_t
        qk = mm(wqkvt[0 : 2 * D, :], u_t).astype(BF16)
        qkvt[t, 0 : 2 * D, :] = qk
        q = qk[0:D, :]
        k = qk[D : 2 * D, :]
        g_lo[...] += mm_nt(q[0:SPLIT, :], k[0:256, :])
        g_hi[...] += mm_nt(q[SPLIT:D, :], k[OFF:D, :])
        qf = q.astype(F32)
        kf = k.astype(F32)
        sq_acc[...] += lane_fold(qf * qf)
        sk_acc[...] += lane_fold(kf * kf)

    for t in range(nb):
        if t == 1:
            for n in range(1, nb):
                x_in(n).wait()
            for n in range(nb):
                dy_in(n).start()
            for i in range(3, 5):
                weight_in(i).wait()
        phase1(t)

    ex_g[0, 0:C, :] = pack(g_lo[...], g_hi[...])
    sq_row = jnp.zeros((1, D), F32)
    sk_row = jnp.zeros((1, D), F32)
    for h in range(H):
        rows = slice(C * h, C * h + C)
        sq_row += to_row(jnp.sum(sq_acc[rows, :], axis=1, keepdims=True), h)
        sk_row += to_row(jnp.sum(sk_acc[rows, :], axis=1, keepdims=True), h)
    ex_g[0, C : C + 8, :] = jnp.concatenate([sq_row, sk_row, jnp.zeros((6, D), F32)], axis=0)
    pl.semaphore_wait(barrier, 7)
    g_core = remote(ex_g.at[0], ex_g.at[1], exg_s.at[0], exg_r.at[0], 1)
    g_chip = remote(ex_h.at[0], ex_h.at[1], exg_s.at[1], exg_r.at[1], 2)
    g_core.start()
    for t in range(nb):
        dy_in(t).wait()

    def gram_step():
        g_core.wait_recv()
        ex_h[0] = ex_g[0] + ex_g[1]
        g_chip.start()

    g_lo[...] = jnp.zeros_like(g_lo)
    g_hi[...] = jnp.zeros_like(g_hi)

    def phase2(t):
        v = mm(wqkvt[2 * D : 3 * D, :], ut[t]).astype(BF16)
        qkvt[t, 2 * D : 3 * D, :] = v
        do = mm_nt(wo_ref[...], dy_v[t]).astype(BF16)
        dot_v[t] = do
        g_lo[...] += mm_nt(do[0:SPLIT, :], v[0:256, :])
        g_hi[...] += mm_nt(do[SPLIT:D, :], v[OFF:D, :])

    for t in range(nb):
        phase2(t)
        if t == 0:
            gram_step()
    ex_a[0] = pack(g_lo[...], g_hi[...])
    for k in range(1, 4):
        small(ex_a, exa_s, exa_r, k).start()

    g_chip.wait_recv()
    gram_all = ex_h[0] + ex_h[1]
    gram = gram_all[0:C, :]
    sq_row = gram_all[C : C + 1, :]
    sk_row = gram_all[C + 1 : C + 2, :]
    rk = lax.rsqrt(sk_row)
    for h in range(H):
        m = col_mask(h)
        rq = lax.rsqrt(to_column(sq_row, h))
        z = jnp.where(m, gram * (tau_ref[h] * rq * rk), -jnp.inf)
        e = jnp.exp(z - jnp.max(z, axis=1, keepdims=True))
        a = e / jnp.sum(e, axis=1, keepdims=True)
        a_f[h] = a
        a_b[C * h : C * h + C, :] = a.astype(BF16)
    a_bt[...] = a_b[...].T

    def phase3(t):
        o_lo, o_hi = block_mm(a_b[...], qkvt[t, 2 * D : 3 * D, :])
        ot[t, 0:SPLIT, :] = o_lo.astype(BF16)
        ot[t, SPLIT:D, :] = o_hi.astype(BF16)

    for t in range(nb):
        phase3(t)
    pw[0] = total(lambda t: mm(ot[t], dy_v[t]))
    start_a(0)

    def phase4(t):
        dv_lo, dv_hi = block_mm(a_bt[...], dot_v[t])
        qkvt[t, 2 * D : 2 * D + SPLIT, :] = dv_lo.astype(BF16)
        qkvt[t, 2 * D + SPLIT : 3 * D, :] = dv_hi.astype(BF16)

    for t in range(nb):
        phase4(t)
    go_on(4, 0)
    pw[1, :, 0:256] = total(lambda t: mm_nt(ut[t], qkvt[t, 2 * D : 2 * D + 256, :]))
    go_on(4, 1)
    pw[1, :, 256:D] = total(lambda t: mm_nt(ut[t], qkvt[t, 2 * D + 256 : 3 * D, :]))
    go_on(4, 2)
    start_a(1)

    for k in range(1, 4):
        small(ex_a, exa_s, exa_r, k).wait_recv()
    go_on(4, 3)
    d_attn = (ex_a[0] + ex_a[1]) + (ex_a[2] + ex_a[3])
    drk = jnp.zeros((1, D), F32)
    lane = lax.broadcasted_iota(jnp.int32, (8, 128), 1)
    dtau = jnp.zeros((8, 128), F32)
    for h in range(H):
        m = col_mask(h)
        tau = tau_ref[h]
        sq = to_column(sq_row, h)
        rq = lax.rsqrt(sq)
        a = a_f[h]
        da = jnp.where(m, d_attn, 0.0)
        dz = a * (da - jnp.sum(da * a, axis=1, keepdims=True))
        dg_b[C * h : C * h + C, :] = jnp.where(m, dz * (tau * rq * rk), 0.0).astype(BF16)
        w = dz * gram
        wrk = jnp.sum(jnp.where(m, w * rk, 0.0), axis=1, keepdims=True)
        dsq = (tau * wrk) * (-0.5 * (rq / sq))
        dsq_v[C * h : C * h + C, :] = jnp.broadcast_to(2.0 * dsq, (C, 128))
        drk += jnp.sum(jnp.where(m, w * (tau * rq), 0.0), axis=0, keepdims=True)
        dtau += jnp.where(lane == h, jnp.sum(wrk * rq), 0.0)
    dsk = drk * (-0.5 * (rk / sk_row))
    for h in range(H):
        dsk_v[C * h : C * h + C, :] = jnp.broadcast_to(2.0 * to_column(dsk, h), (C, 128))
    dg_bt[...] = dg_b[...].T
    ex_t[0] = dtau
    t_copy = remote(ex_t.at[0], ex_t.at[1], t_s, t_r, 4)
    t_copy.start()

    def phase5(t):
        dq_lo, dq_hi = block_mm(dg_b[...], qkvt[t, D : 2 * D, :])
        qf = qkvt[t, 0:D, :].astype(F32)
        ds = dsq_v[:, 0:1]
        dot_v[t, 0:SPLIT, :] = (dq_lo + ds[0:SPLIT] * qf[0:SPLIT]).astype(BF16)
        dot_v[t, SPLIT:D, :] = (dq_hi + ds[SPLIT:D] * qf[SPLIT:D]).astype(BF16)

    for t in range(nb):
        phase5(t)
    go_on(5, 0)
    pw[2, :, 0:256] = total(lambda t: mm_nt(ut[t], dot_v[t, 0:256, :]))
    go_on(5, 1)
    pw[2, :, 256:D] = total(lambda t: mm_nt(ut[t], dot_v[t, 256:D, :]))
    go_on(5, 2)
    start_a(2)

    def phase6(t):
        dk_lo, dk_hi = block_mm(dg_bt[...], qkvt[t, 0:D, :])
        kf = qkvt[t, D : 2 * D, :].astype(F32)
        ds = dsk_v[:, 0:1]
        qkvt[t, D : D + SPLIT, :] = (dk_lo + ds[0:SPLIT] * kf[0:SPLIT]).astype(BF16)
        qkvt[t, D + SPLIT : 2 * D, :] = (dk_hi + ds[SPLIT:D] * kf[SPLIT:D]).astype(BF16)

    for t in range(nb):
        phase6(t)
    go_on(6, 0)
    pw[3, :, 0:256] = total(lambda t: mm_nt(ut[t], qkvt[t, D : D + 256, :]))
    go_on(6, 1)
    pw[3, :, 256:D] = total(lambda t: mm_nt(ut[t], qkvt[t, D + 256 : 2 * D, :]))
    go_on(6, 2)
    start_a(3)

    def phase7(t, half):
        rows = slice(half * (TB // 2), (half + 1) * (TB // 2))
        du_t = mm(wqkv_ref[:, 0:D], dot_v[t, :, rows]) + mm(wqkv_ref[:, D : 3 * D], qkvt[t, D : 3 * D, rows])
        du = du_t.astype(BF16).T.astype(F32)
        rstd = rstd_v[t, rows, 0:1]
        xhat = (x_v[t, rows].astype(F32) - mean_v[t, rows, 0:1]) * rstd
        g = du * gamma
        m1 = jnp.mean(g, axis=-1, keepdims=True)
        m2 = jnp.mean(g * xhat, axis=-1, keepdims=True)
        dx = rstd * (g - m1 - xhat * m2)
        dx_v[t, rows] = (dy_v[t, rows].astype(F32) + dx).astype(BF16)
        gb_acc[0] += jnp.sum((du * xhat).reshape(TB // 16, 8, D), axis=0)
        gb_acc[1] += jnp.sum(du.reshape(TB // 16, 8, D), axis=0)

    for t in range(nb):
        for half in range(2):
            phase7(t, half)
            go_on(7, t, half)

    dgam = jnp.sum(gb_acc[0], axis=0, keepdims=True)
    dbet = jnp.sum(gb_acc[1], axis=0, keepdims=True)
    ex_gb[0] = jnp.concatenate([dgam, dbet, jnp.zeros((6, D), F32)], axis=0)
    for k in range(1, 8):
        small(ex_gb, gb_s, gb_r, k).start()

    def phase8(t):
        y_v[t] = (x_v[t].astype(F32) + mm(ot[t].T, wo_ref[...])).astype(BF16)

    for t in range(nb):
        phase8(t)
        go_on(8, t, 1)

    for c in range(4):
        for h in range(PIECES[c]):
            stage_c(c, h).wait_recv()
        both = sb[c] + rc[c]
        if c == 0:
            gwo_ref[...] = both
        else:
            col = {1: 2 * D, 2: 0, 3: D}[c]
            gwqkv_ref[:, col : col + D] = both
    t_copy.wait_recv()
    gtau_ref[...] = (ex_t[0] + ex_t[1])[0, 0:H]
    for k in range(1, 8):
        small(ex_gb, gb_s, gb_r, k).wait_recv()
    gb = ((ex_gb[0] + ex_gb[1]) + (ex_gb[2] + ex_gb[3])) + ((ex_gb[4] + ex_gb[5]) + (ex_gb[6] + ex_gb[7]))
    ggam_ref[...] = gb[0]
    gbet_ref[...] = gb[1]

    for k in range(1, 4):
        small(ex_a, exa_s, exa_r, k).wait_send()
    for c in range(4):
        for xx in range(2):
            stage_a(c, xx).wait_send()
        for h in range(PIECES[c]):
            stage_b(c, h).wait_send()
            stage_c(c, h).wait_send()
    g_core.wait_send()
    g_chip.wait_send()
    t_copy.wait_send()
    for k in range(1, 8):
        small(ex_gb, gb_s, gb_r, k).wait_send()


def store_kernel(*refs):
    sem = refs[14]
    copies = []
    for i in range(7):
        src, dst = refs[i], refs[7 + i]
        for at in range(src.shape[0]) if i < 2 else [None]:
            pair = (src, dst) if at is None else (src.at[at], dst.at[at])
            copies.append(pltpu.make_async_copy(*pair, sem.at[len(copies)]))
    for copy in copies:
        copy.start()
    for copy in copies:
        copy.wait()


def solution(mesh):
    act_spec = P(("data", "img"), "seq", None)
    row_spec = P(("data", "seq"), None)
    in_specs = (act_spec, act_spec, P(), P(), P(), P(), P())
    out_specs = (act_spec, act_spec, row_spec, row_spec, P("data"), P("data"), P("data"))

    def local_block(x_in, grad_y, ln_gamma, ln_beta, w_qkv, w_out, head_temp):
        n_tok = x_in.shape[1]
        nb = n_tok // TB
        hbm = pl.BlockSpec(memory_space=pl.ANY)
        vmem = pl.BlockSpec(memory_space=pltpu.VMEM)
        dma = pltpu.SemaphoreType.DMA
        outs = pl.pallas_call(
            functools.partial(kernel, nb),
            out_shape=(
                pltpu.VMEM((nb, TB, D), BF16),
                pltpu.VMEM((nb, TB, D), BF16),
                pltpu.VMEM((ROWS, 3 * D), F32),
                pltpu.VMEM((ROWS, D), F32),
                pltpu.VMEM((D,), F32),
                pltpu.VMEM((D,), F32),
                pltpu.VMEM((H,), F32),
            ),
            in_specs=[hbm] * 7,
            out_specs=(vmem,) * 7,
            scratch_shapes=[
                pltpu.VMEM((nb, TB, D), BF16),
                pltpu.VMEM((nb, TB, D), BF16),
                pltpu.VMEM((nb, D, TB), BF16),
                pltpu.VMEM((nb, 3 * D, TB), BF16),
                pltpu.VMEM((nb, D, TB), BF16),
                pltpu.VMEM((nb, D, TB), BF16),
                pltpu.VMEM((nb, TB, 128), F32),
                pltpu.VMEM((nb, TB, 128), F32),
                pltpu.VMEM((3 * D, D), BF16),
                pltpu.VMEM((D,), F32),
                pltpu.VMEM((D,), F32),
                pltpu.VMEM((D, 3 * D), BF16),
                pltpu.VMEM((D, D), BF16),
                pltpu.SMEM((H,), F32),
                pltpu.VMEM((SPLIT, 256), F32),
                pltpu.VMEM((D - SPLIT, 256), F32),
                pltpu.VMEM((D, 128), F32),
                pltpu.VMEM((D, 128), F32),
                pltpu.VMEM((2, C + 8, D), F32),
                pltpu.VMEM((2, C + 8, D), F32),
                pltpu.VMEM((4, C, D), F32),
                pltpu.VMEM((H, C, D), F32),
                pltpu.VMEM((D, D), BF16),
                pltpu.VMEM((D, D), BF16),
                pltpu.VMEM((D, D), BF16),
                pltpu.VMEM((D, D), BF16),
                pltpu.VMEM((D, 128), F32),
                pltpu.VMEM((D, 128), F32),
                pltpu.VMEM((4, D, D), F32),
                pltpu.VMEM((4, 2, ROWS, D), F32),
                pltpu.VMEM((4, 2, ROWS, D), F32),
                pltpu.VMEM((4, ROWS, D), F32),
                pltpu.VMEM((4, ROWS, D), F32),
                pltpu.VMEM((4, ROWS, D), F32),
                pltpu.VMEM((2, 8, D), F32),
                pltpu.VMEM((8, 8, D), F32),
                pltpu.VMEM((2, 8, 128), F32),
                dma((nb,)), dma((nb,)), dma((5,)),
                dma((2,)), dma((2,)), dma((4,)), dma((4,)),
                dma((4, 2)), dma((4, 2)), dma((4, max(PIECES))), dma((4, max(PIECES))), dma((4, max(PIECES))), dma((4, max(PIECES))),
                dma((8,)), dma((8,)), dma, dma,
            ],
            compiler_params=pltpu.CompilerParams(
                collective_id=0, has_side_effects=True, vmem_limit_bytes=52000000
            ),
            name="xca_block",
        )(
            x_in.reshape(nb, TB, D),
            grad_y.reshape(nb, TB, D),
            ln_gamma,
            ln_beta,
            w_qkv,
            w_out,
            head_temp,
        )
        outs = pl.pallas_call(
            store_kernel,
            out_shape=(
                jax.ShapeDtypeStruct((nb, TB, D), BF16),
                jax.ShapeDtypeStruct((nb, TB, D), BF16),
                jax.ShapeDtypeStruct((ROWS, 3 * D), F32),
                jax.ShapeDtypeStruct((ROWS, D), F32),
                jax.ShapeDtypeStruct((D,), F32),
                jax.ShapeDtypeStruct((D,), F32),
                jax.ShapeDtypeStruct((H,), F32),
            ),
            in_specs=[hbm] * 7,
            out_specs=(hbm,) * 7,
            scratch_shapes=[dma((2 * nb + 5,))],
            compiler_params=pltpu.CompilerParams(vmem_limit_bytes=4 * 2**20),
            name="xca_store",
        )(*outs)
        y, dx, gwqkv, gwo, ggam, gbet, gtau = outs
        return y.reshape(1, n_tok, D), dx.reshape(1, n_tok, D), gwqkv, gwo, ggam, gbet, gtau

    return jax.shard_map(local_block, mesh=mesh, in_specs=in_specs, out_specs=out_specs, check_vma=False)
```
